16 devices in a mesh: data: 4 (over z, y), sp: 4 (over x, core).
Axes of the slice: x: 2, y: 2, z: 2, core: 2. Of those that a mesh axis runs over, the one named last changes fastest.
Arguments:
- latent: bfloat16 [4, 128, 256, 384], P('data', 'sp'), parts along dimension 0
- ln_gain: bfloat16 [4, 384], replicated
- ln_bias: bfloat16 [4, 384], replicated
- w_qkv: bfloat16 [2, 384, 3, 6, 64], replicated
- w_out: bfloat16 [2, 6, 64, 384], replicated
- w_up: bfloat16 [2, 384, 1536], replicated
- w_down: bfloat16 [2, 1536, 384], replicated
Outputs:
- output: bfloat16 [4, 128, 256, 384], P('data', 'sp'), parts along dimension 0
There are 4 independent parts. The reference program is written for one: setup_inputs(seed, part) draws one part's arguments, and reference() takes and returns one part's arrays. A program takes and returns all parts, laid end to end along the dimension named above; an argument that names none is the same for every part.
All inputs are finite; a program needn't handle non-finite values.
Results may differ from the reference program's by a relative error of at most 0.0114142.
Values are sent between devices in bfloat16 or wider.
A program may use at most 1 GiB of HBM per device.

```python
import jax
import jax.numpy as jnp
from jax import lax
from functools import partial

FRAMES = 128
PATCHES = 256
WIDTH = 384
NUM_HEADS = 6
HEAD_DIM = WIDTH // NUM_HEADS
LN_EPS = 1e-6


def setup_inputs(seed: int = 0, part: int = 0) -> dict:
    part_key = jax.random.fold_in(jax.random.key(seed), part)
    noise_key, frame_key, patch_key = jax.random.split(part_key, 3)
    noise = jax.random.normal(noise_key, (1, FRAMES, PATCHES, WIDTH), jnp.float32)
    frame_sig = jax.random.normal(frame_key, (1, FRAMES, 1, WIDTH), jnp.float32)
    patch_sig = jax.random.normal(patch_key, (1, 1, PATCHES, WIDTH), jnp.float32)
    latent = 0.6 * noise + frame_sig + 0.8 * patch_sig
    weight_keys = jax.random.split(jax.random.key(seed + 1), 6)
    qk_boost = jnp.array([1.3, 1.3, 1.0], jnp.float32).reshape(1, 1, 3, 1, 1)
    ln_gain = 1.0 + 0.4 * jax.random.normal(weight_keys[0], (4, WIDTH), jnp.float32)
    ln_bias = 0.5 * jax.random.normal(weight_keys[1], (4, WIDTH), jnp.float32)
    w_qkv = jax.random.normal(weight_keys[2], (2, WIDTH, 3, NUM_HEADS, HEAD_DIM), jnp.float32) * qk_boost * WIDTH ** -0.5
    w_out = jax.random.normal(weight_keys[3], (2, NUM_HEADS, HEAD_DIM, WIDTH), jnp.float32) * WIDTH ** -0.5
    w_up = jax.random.normal(weight_keys[4], (2, WIDTH, 4 * WIDTH), jnp.float32) * WIDTH ** -0.5
    w_down = jax.random.normal(weight_keys[5], (2, 4 * WIDTH, WIDTH), jnp.float32) * (4 * WIDTH) ** -0.5
    return {
        'latent': latent.astype(jnp.bfloat16),
        'ln_gain': ln_gain.astype(jnp.bfloat16),
        'ln_bias': ln_bias.astype(jnp.bfloat16),
        'w_qkv': w_qkv.astype(jnp.bfloat16),
        'w_out': w_out.astype(jnp.bfloat16),
        'w_up': w_up.astype(jnp.bfloat16),
        'w_down': w_down.astype(jnp.bfloat16),
    }


def layer_norm(tokens, gain_vec, shift_vec):
    as_float = tokens.astype(jnp.float32)
    mean_val = jnp.mean(as_float, axis=-1, keepdims=True)
    centered = as_float - mean_val
    variance = jnp.mean(centered * centered, axis=-1, keepdims=True)
    normed = centered * lax.rsqrt(variance + LN_EPS) * gain_vec.astype(jnp.float32) + shift_vec.astype(jnp.float32)
    return normed.astype(jnp.bfloat16)


def seq_block(sequence, layer_idx, ln_gain, ln_bias, w_qkv, w_out, w_up, w_down):
    length = sequence.shape[0]
    normed = layer_norm(sequence, ln_gain[2 * layer_idx], ln_bias[2 * layer_idx])
    qkv_all = jnp.dot(normed, w_qkv[layer_idx].reshape(WIDTH, 3 * WIDTH), preferred_element_type=jnp.float32).astype(jnp.bfloat16)
    qkv_all = qkv_all.reshape(length, 3, NUM_HEADS, HEAD_DIM).astype(jnp.float32)
    scores = jnp.einsum('qhk,phk->hqp', qkv_all[:, 0], qkv_all[:, 1]) * HEAD_DIM ** -0.5
    attn_probs = jax.nn.softmax(scores, axis=-1).astype(jnp.bfloat16)
    attended = jnp.einsum('hqp,phk->qhk', attn_probs.astype(jnp.float32), qkv_all[:, 2]).astype(jnp.bfloat16)
    projected = jnp.dot(attended.reshape(length, WIDTH), w_out[layer_idx].reshape(WIDTH, WIDTH), preferred_element_type=jnp.float32)
    residual = (sequence.astype(jnp.float32) + projected).astype(jnp.bfloat16)
    normed_mlp = layer_norm(residual, ln_gain[2 * layer_idx + 1], ln_bias[2 * layer_idx + 1])
    hidden = jax.nn.gelu(jnp.dot(normed_mlp, w_up[layer_idx], preferred_element_type=jnp.float32), approximate=True).astype(jnp.bfloat16)
    result = residual.astype(jnp.float32) + jnp.dot(hidden, w_down[layer_idx], preferred_element_type=jnp.float32)
    return result.astype(jnp.bfloat16)


def reference(latent, ln_gain, ln_bias, w_qkv, w_out, w_up, w_down):
    space_fn = partial(seq_block, layer_idx=0, ln_gain=ln_gain, ln_bias=ln_bias, w_qkv=w_qkv, w_out=w_out, w_up=w_up, w_down=w_down)
    spatial = lax.map(space_fn, latent[0])
    time_fn = partial(seq_block, layer_idx=1, ln_gain=ln_gain, ln_bias=ln_bias, w_qkv=w_qkv, w_out=w_out, w_up=w_up, w_down=w_down)
    temporal = lax.map(time_fn, jnp.swapaxes(spatial, 0, 1))
    return jnp.swapaxes(temporal, 0, 1)[None]
```

```python
import functools

import jax
import jax.numpy as jnp
from jax import lax
from jax.experimental import pallas as pl
from jax.experimental.pallas import tpu as pltpu
from jax.sharding import PartitionSpec as P

BF, F32 = jnp.bfloat16, jnp.float32
D, H, DH, F = 384, 6, 64, 1536
T = 256
EPS = 1e-6
C_EXP = 0.125 * 1.4426950408889634
G0, G1 = 0.7978845608028654, 0.044715
RB = 64
NSLOT = 4
MESH_ID = pl.DeviceIdType.MESH


def dot(a, b):
    return jnp.dot(a, b, preferred_element_type=F32)


def psum(v):
    return jnp.sum(v.reshape(v.shape[0] // 8, 8, v.shape[1]), axis=0)


def dup(r):
    return jnp.concatenate([r, r], axis=1)


def full_mean(acc):
    return jnp.sum(acc, axis=0, keepdims=True) * (1.0 / D)


def gelu_of_half(z):
    return (z + z * jnp.tanh(z * (z * z * (8 * G0 * G1) + 2 * G0))).astype(BF)


def ln_p1(xn, x_ring, xf_s):
    x_ring[...] = xn
    acc = None
    for r in range(0, D, RB):
        f = xn[r:r + RB].astype(F32)
        xf_s[pl.ds(r, RB), :] = f
        t = psum(f)
        acc = t if acc is None else acc + t
    return full_mean(acc)


def ln2_p1(x_ring, pr, hf_s):
    acc = None
    for r in range(0, D, RB):
        f = (x_ring[pl.ds(r, RB), :].astype(F32) + pr[r:r + RB]).astype(BF).astype(F32)
        hf_s[pl.ds(r, RB), :] = f
        t = psum(f)
        acc = t if acc is None else acc + t
    return full_mean(acc)


def ln_p2(f_s, mean):
    acc = None
    for r in range(0, D, RB):
        c = f_s[pl.ds(r, RB), :] - mean
        t = psum(c * c)
        acc = t if acc is None else acc + t
    return lax.rsqrt(full_mean(acc) + EPS)


def ln_p3(f_s, mean, rstd, g_ref, b_ref, out):
    for r in range(0, D, RB):
        c = f_s[pl.ds(r, RB), :] - mean
        out[pl.ds(r, RB), :] = (c * rstd * dup(g_ref[pl.ds(r, RB), :]) + dup(b_ref[pl.ds(r, RB), :])).astype(BF)


def softmax_half(s):
    m = jnp.max(s, axis=0, keepdims=True)
    e = jnp.exp2((s - m) * C_EXP)
    return e.astype(BF), jnp.sum(e, axis=0, keepdims=True)


def setup_weights(gain_ref, bias_ref, wout_ref, wup_ref, wdown_ref, wo_s, wu_s, wd_s, gb_s, layer):
    wo_s[...] = wout_ref[0].T
    wu_s[...] = wup_ref[0].T * 0.5
    wd_s[...] = wdown_ref[0].T
    for i, r in enumerate((gain_ref, bias_ref)):
        for j in range(2):
            row = r[pl.ds(2 * layer + j, 1), :].astype(F32)
            gb_s[2 * i + j] = jnp.broadcast_to(row, (128, D)).T


def block_step(i, layer, xn, wqkv, wo_s, wu_s, wd_s, gb_s, x_s, a_s, qkv_s, o_s, u_s, a2_s, xf_s, hf_s):
    cur = jnp.bitwise_and(i, 1)
    nxt = 1 - cur
    zs, ss, es, os = {}, {}, {}, {}
    qc, qn = qkv_s.at[cur], qkv_s.at[nxt]
    an, a_out = a_s.at[nxt], a_s.at[cur]
    op, on = o_s.at[nxt], o_s.at[cur]

    def up(j):
        zs[j] = [dot(wu_s[pl.ds(256 * j + 128 * t, 128), :], a2_s[...]) for t in range(2)]

    def act(j):
        for t, z in enumerate(zs.pop(j)):
            u_s[pl.ds(256 * j + 128 * t, 128), :] = gelu_of_half(z)

    def lanes(h):
        return pl.ds(128 * (h // 3), 128)

    def S(h):
        if layer == 0:
            ss[h] = dot(qc[pl.ds(D + h * DH, DH), :].T, qc[pl.ds(h * DH, DH), :])
        else:
            c, r = lanes(h), 128 * (h % 3)
            q0, q1 = qc[pl.ds(r, 64), c], qc[pl.ds(r + 64, 64), c]
            z = jnp.zeros_like(q0)
            q = jnp.concatenate([jnp.concatenate([q0, z], axis=1), jnp.concatenate([z, q1], axis=1)], axis=0)
            ss[h] = dot(qc[pl.ds(D + r, 128), c].T, q)

    def Pm(h):
        s = ss.pop(h)
        e0, l0 = softmax_half(s[:, :128])
        e1, l1 = softmax_half(s[:, 128:])
        es[h] = (jnp.concatenate([e0, e1], axis=1), jnp.concatenate([l0, l1], axis=1))

    def PV(h):
        if layer == 0:
            os[h] = dot(qc[pl.ds(2 * D + h * DH, DH), :], es[h][0])
        else:
            os[h] = dot(qc[pl.ds(2 * D + 128 * (h % 3), 128), lanes(h)], es[h][0])

    def OS(h):
        o, r = os.pop(h), 1.0 / es.pop(h)[1]
        if layer == 0:
            on[pl.ds(h * DH, DH), :] = (o * r).astype(BF)
        else:
            k, c = 128 * (h % 3), lanes(h)
            on[pl.ds(k, 64), c] = (o[:64, :128] * r[:, :128]).astype(BF)
            on[pl.ds(k + 64, 64), c] = (o[64:, 128:] * r[:, 128:]).astype(BF)

    def Q(c):
        for t in range(2):
            qn[pl.ds(c * D + 192 * t, 192), :] = dot(wqkv[0, pl.ds(c * D + 192 * t, 192), :], an[...]).astype(BF)

    def dn(k):
        return [dot(wd_s[pl.ds(192 * t, 192), 256 * k:256 * k + 256], u_s[pl.ds(256 * k, 256), :]) for t in range(2)]

    def addl(*parts):
        return [functools.reduce(lambda a, b: a + b, z) for z in zip(*parts)]

    pr = jnp.concatenate([dot(wo_s[pl.ds(192 * t, 192), :], op[...]) for t in range(2)], axis=0)
    S(0)
    Q(0)
    mean2 = ln2_p1(x_s.at[jnp.bitwise_and(i + 3, 3)], pr, hf_s)
    S(1); Pm(0)
    rstd2 = ln_p2(hf_s, mean2)
    Q(1)
    ln_p3(hf_s, mean2, rstd2, gb_s.at[1], gb_s.at[3], a2_s)
    PV(0)
    up(0)
    Pm(1)
    Q(2)
    S(2)
    up(1); act(0)
    OS(0); PV(1)
    up(2); act(1)
    Pm(2); S(3); up(3)
    PV(2); OS(1); act(2)
    Pm(3); S(4); up(4)
    PV(3); OS(2); act(3)
    Pm(4); S(5); up(5)
    PV(4); OS(3); act(4)
    Pm(5)
    yd = addl(dn(0), dn(1))
    PV(5); OS(4); act(5)
    yd = addl(yd, dn(2), dn(3))
    mean1 = ln_p1(xn(), x_s.at[jnp.bitwise_and(i + 2, 3)], xf_s)
    OS(5)
    rstd1 = ln_p2(xf_s, mean1)
    yd = addl(yd, dn(4), dn(5))
    ln_p3(xf_s, mean1, rstd1, gb_s.at[0], gb_s.at[2], a_out)
    y = hf_s[...] + jnp.concatenate(yd, axis=0)
    return y.T.astype(BF)


def prologue(xns, wqkv, gb_s, x_s, a_s, qkv_s, o_s, xf_s):
    for t in range(2):
        mean = ln_p1(xns[t](), x_s.at[t], xf_s)
        ln_p3(xf_s, mean, ln_p2(xf_s, mean), gb_s.at[0], gb_s.at[2], a_s.at[t])
    qkv_s[0] = dot(wqkv[0], a_s[0]).astype(BF)
    o_s[...] = jnp.zeros_like(o_s)
    x_s[3] = jnp.zeros((D, T), BF)


def greet(axis, n):
    me = lax.axis_index(axis)
    barrier = pltpu.get_barrier_semaphore()
    for k in range(1, n):
        pl.semaphore_signal(barrier, inc=1, device_id={axis: lax.rem(me + k, n)}, device_id_type=MESH_ID)
    pl.semaphore_wait(barrier, n - 1)


def exchange(axis, n, src, dst, local_sem, send_sem, recv_sem):
    me = lax.axis_index(axis)
    out = [pltpu.make_async_copy(src(me), dst, local_sem)]
    for k in range(1, n):
        to = lax.rem(me + k, n)
        out.append(pltpu.make_async_remote_copy(
            src_ref=src(to), dst_ref=dst, send_sem=send_sem.at[k - 1], recv_sem=recv_sem.at[k - 1],
            device_id={axis: to}, device_id_type=MESH_ID))
    return out


def send_step(i, steps, axis, n, y, ybuf, tile_copies, local_sem, send_sem, recv_sem, recv_part):
    f = i - 1
    slot = lax.rem(i + NSLOT - 1, NSLOT)

    @pl.when(f >= NSLOT)
    def _():
        cs = tile_copies(f - NSLOT, slot)
        cs[0].wait()
        for c in cs[1:]:
            c.wait_send()

    y()

    @pl.when(f >= 0)
    def _():
        for c in tile_copies(f, slot):
            c.start()

    @pl.when(f == steps - 1)
    def _():
        for b in range(NSLOT):
            g = steps - NSLOT + b
            cs = tile_copies(g, g % NSLOT)
            cs[0].wait()
            for c in cs[1:]:
                c.wait_send()
        for k in range(n - 1):
            pltpu.make_async_copy(recv_part, recv_part, recv_sem.at[k]).wait()


def space_kernel(axis, n, steps, xn_ref, gain_ref, bias_ref, wqkv, wout_ref, wup_ref, wdown_ref, x0_ref, z_ref,
                 wo_s, wu_s, wd_s, gb_s, x_s, a_s, qkv_s, o_s, u_s, a2_s, xf_s, hf_s, ybuf, local_sem, send_sem, recv_sem):
    i = pl.program_id(0)
    me = lax.axis_index(axis)
    part = T // n

    @pl.when(i == 0)
    def _():
        greet(axis, n)
        setup_weights(gain_ref, bias_ref, wout_ref, wup_ref, wdown_ref, wo_s, wu_s, wd_s, gb_s, 0)
        prologue([lambda: x0_ref[0].T, lambda: x0_ref[1].T], wqkv, gb_s, x_s, a_s, qkv_s, o_s, xf_s)

    def tile_copies(f, slot):
        return exchange(axis, n, lambda k: ybuf.at[slot, pl.ds(pl.multiple_of(part * k, part), part)],
                        z_ref.at[me * steps + f], local_sem.at[slot], send_sem.at[slot], recv_sem)

    def y():
        ybuf[lax.rem(i + NSLOT - 1, NSLOT)] = block_step(
            i, 0, lambda: xn_ref[0].T, wqkv, wo_s, wu_s, wd_s, gb_s, x_s, a_s, qkv_s, o_s, u_s, a2_s, xf_s, hf_s)

    send_step(i, steps, axis, n, y, ybuf, tile_copies, local_sem, send_sem, recv_sem, z_ref.at[pl.ds(0, steps)])


def time_kernel(axis, n, steps, zn_ref, gain_ref, bias_ref, wqkv, wout_ref, wup_ref, wdown_ref, z0_ref, w_ref,
                wo_s, wu_s, wd_s, gb_s, x_s, a_s, qkv_s, o_s, u_s, a2_s, xf_s, hf_s, ybuf, local_sem, send_sem, recv_sem, c_s):
    i = pl.program_id(0)
    me = lax.axis_index(axis)
    part = 128 // n

    def convert(z, chunk, q):
        v = z.astype(F32).reshape(256, D)
        for j in range(3):
            c_s[chunk, j, pl.ds(pl.multiple_of(256 * q, 256), 256), :] = v[:, 128 * j:128 * j + 128]

    def tile(chunk, pair):
        return jnp.concatenate([
            jnp.concatenate([c_s[chunk, j, pl.ds(2 * pair + t, 128, stride=8), :].astype(BF).T for t in range(2)], axis=1)
            for j in range(3)], axis=0)

    @pl.when(i == 0)
    def _():
        greet(axis, n)
        setup_weights(gain_ref, bias_ref, wout_ref, wup_ref, wdown_ref, wo_s, wu_s, wd_s, gb_s, 1)
        for q in range(4):
            convert(z0_ref[pl.ds(32 * q, 32), pl.ds(0, 8), :], 0, q)
        for q in range(2):
            convert(z0_ref[pl.ds(32 * q, 32), pl.ds(8, 8), :], 1, q)
        prologue([lambda: tile(0, 0), lambda: tile(0, 1)], wqkv, gb_s, x_s, a_s, qkv_s, o_s, xf_s)

    def tile_copies(f, slot):
        return exchange(axis, n, lambda k: ybuf.at[slot, :, pl.ds(pl.multiple_of(part * k, part), part)],
                        w_ref.at[pl.ds(2 * (me * steps + f), 2)], local_sem.at[slot], send_sem.at[slot], recv_sem)

    def y():
        t = i + 2
        q = jnp.bitwise_and(t, 3)
        chunk = jnp.bitwise_and(lax.shift_right_logical(t, 2), 1)
        out = block_step(
            i, 1, lambda: tile(chunk, q), wqkv, wo_s, wu_s, wd_s, gb_s, x_s, a_s, qkv_s, o_s, u_s, a2_s, xf_s, hf_s)
        ybuf[lax.rem(i + NSLOT - 1, NSLOT)] = out.reshape(2, 128, D)
        convert(zn_ref[pl.ds(pl.multiple_of(32 * q, 32), 32)], 1 - chunk, q)

    send_step(i, steps, axis, n, y, ybuf, tile_copies, local_sem, send_sem, recv_sem, w_ref.at[pl.ds(0, 2 * steps)])


def swap_kernel(w_ref, out_ref, s_ref):
    k = w_ref.shape[0]
    v = w_ref[...].astype(F32).reshape(k * 32, D)
    for j in range(3):
        s_ref[j] = v[:, 128 * j:128 * j + 128]
    for f in range(32):
        for j in range(3):
            out_ref[f, :, 128 * j:128 * j + 128] = s_ref[j, pl.ds(f, k, stride=32), :].astype(BF)


def weight_spec(shape, layer):
    return pl.BlockSpec((1,) + shape, lambda i: (layer, 0, 0), pipeline_mode=pl.Buffered(1))


def solution(mesh):
    axis = 'sp'
    n = mesh.shape[axis]
    steps = 32
    act_spec = P('data', axis, None, None)

    def block(kernel, layer, x, xspec, x0spec, out_shape, ybuf, weights, extra):
        small = pl.BlockSpec((4, D), lambda i: (0, 0), pipeline_mode=pl.Buffered(1))
        flops = 2 * steps * T * (3 * D * D + D * D + 2 * D * F + 2 * D * T)
        return pl.pallas_call(
            functools.partial(kernel, axis, n, steps),
            grid=(steps + 1,),
            out_shape=out_shape,
            in_specs=[xspec, small, small, weight_spec((3 * D, D), layer), weight_spec((D, D), layer),
                      weight_spec((D, F), layer), weight_spec((F, D), layer), x0spec],
            out_specs=pl.BlockSpec(memory_space=pl.ANY),
            scratch_shapes=[
                pltpu.VMEM((D, D), BF), pltpu.VMEM((F, D), BF), pltpu.VMEM((D, F), BF),
                pltpu.VMEM((4, D, 128), F32),
                pltpu.VMEM((4, D, T), BF), pltpu.VMEM((2, D, T), BF),
                pltpu.VMEM((2, 3 * D, T), BF), pltpu.VMEM((2, D, T), BF), pltpu.VMEM((F, T), BF),
                pltpu.VMEM((D, T), BF),
                pltpu.VMEM((D, T), F32), pltpu.VMEM((D, T), F32),
                ybuf,
                pltpu.SemaphoreType.DMA((NSLOT,)), pltpu.SemaphoreType.DMA((NSLOT, n - 1)), pltpu.SemaphoreType.DMA((n - 1,)),
            ] + extra,
            compiler_params=pltpu.CompilerParams(
                dimension_semantics=("arbitrary",), vmem_limit_bytes=60 << 20,
                collective_id=layer, has_side_effects=True),
            cost_estimate=pl.CostEstimate(flops=flops, bytes_accessed=4 * steps * T * D, transcendentals=0),
            name=('space_block', 'time_block')[layer],
        )(x, *weights, x)

    def local_run(latent, ln_gain, ln_bias, w_qkv, w_out, w_up, w_down):
        weights = (ln_gain, ln_bias, jnp.transpose(w_qkv, (0, 2, 3, 4, 1)).reshape(2, 3 * D, D), w_out.reshape(2, D, D), w_up, w_down)
        x = latent[0]
        z = block(
            space_kernel, 0, x,
            pl.BlockSpec((1, T, D), lambda i: (jnp.minimum(i + 2, steps - 1), 0, 0)),
            pl.BlockSpec((2, T, D), lambda i: (0, 0, 0), pipeline_mode=pl.Buffered(1)),
            jax.ShapeDtypeStruct((128, 64, D), BF), pltpu.VMEM((NSLOT, T, D), BF), weights, [])
        w = block(
            time_kernel, 1, z,
            pl.BlockSpec((128, 8, D), lambda i: (0, jnp.minimum((i + 6) // 4, 7), 0)),
            pl.BlockSpec((128, 16, D), lambda i: (0, 0, 0), pipeline_mode=pl.Buffered(1)),
            jax.ShapeDtypeStruct((256, 32, D), BF), pltpu.VMEM((NSLOT, 2, 128, D), BF), weights,
            [pltpu.VMEM((2, 3, 1024, 128), F32)])
        out = pl.pallas_call(
            swap_kernel,
            grid=(16,),
            out_shape=jax.ShapeDtypeStruct((32, 256, D), BF),
            in_specs=[pl.BlockSpec((16, 32, D), lambda i: (i, 0, 0))],
            out_specs=pl.BlockSpec((32, 16, D), lambda i: (0, i, 0)),
            scratch_shapes=[pltpu.VMEM((3, 16 * 32, 128), F32)],
            name='swap',
        )(w)
        return out[None]

    return jax.shard_map(local_run, mesh=mesh, in_specs=(act_spec, P(), P(), P(), P(), P(), P()), out_specs=act_spec, check_vma=False)
```

```python
import functools

import jax
import jax.numpy as jnp
from jax import lax
from jax.experimental import pallas as pl
from jax.experimental.pallas import tpu as pltpu
from jax.sharding import PartitionSpec as P

BF, F32 = jnp.bfloat16, jnp.float32
D, H, DH, F = 384, 6, 64, 1536
T = 256
EPS = 1e-6
C_EXP = 0.125 * 1.4426950408889634
G0, G1 = 0.7978845608028654, 0.044715
RB = 64
MESH_ID = pl.DeviceIdType.MESH


def band(a, b):
    return a & b if isinstance(a, int) else jnp.bitwise_and(a, b)


def dot(a, b):
    return jnp.dot(a, b, preferred_element_type=F32)


def psum(v):
    return jnp.sum(v.reshape(v.shape[0] // 8, 8, v.shape[1]), axis=0)


def dup(r):
    return jnp.concatenate([r, r], axis=1)


def full_mean(acc):
    return jnp.sum(acc, axis=0, keepdims=True) * (1.0 / D)


def gelu_of_half(z):
    return (z + z * jnp.tanh(z * (z * z * (8 * G0 * G1) + 2 * G0))).astype(BF)


def ln_p1(xn, x_ring, xf_s):
    x_ring[...] = xn
    acc = None
    for r in range(0, D, RB):
        f = xn[r:r + RB].astype(F32)
        xf_s[pl.ds(r, RB), :] = f
        t = psum(f)
        acc = t if acc is None else acc + t
    return full_mean(acc)


def ln2_p1(x_ring, pr, hf_s):
    acc = None
    for r in range(0, D, RB):
        f = (x_ring[pl.ds(r, RB), :].astype(F32) + pr[r:r + RB]).astype(BF).astype(F32)
        hf_s[pl.ds(r, RB), :] = f
        t = psum(f)
        acc = t if acc is None else acc + t
    return full_mean(acc)


def ln_p2(f_s, mean):
    acc = None
    for r in range(0, D, RB):
        c = f_s[pl.ds(r, RB), :] - mean
        t = psum(c * c)
        acc = t if acc is None else acc + t
    return lax.rsqrt(full_mean(acc) + EPS)


def ln_p3(f_s, mean, rstd, g_ref, b_ref, out):
    for r in range(0, D, RB):
        c = f_s[pl.ds(r, RB), :] - mean
        out[pl.ds(r, RB), :] = (c * rstd * dup(g_ref[pl.ds(r, RB), :]) + dup(b_ref[pl.ds(r, RB), :])).astype(BF)


def softmax_half(s):
    m = jnp.max(s, axis=0, keepdims=True)
    e = jnp.exp2((s - m) * C_EXP)
    return e.astype(BF), jnp.sum(e, axis=0, keepdims=True)


def norm_rows(gain_ref, bias_ref, gb_s, layer):
    for i, r in enumerate((gain_ref, bias_ref)):
        for j in range(2):
            row = r[pl.ds(2 * layer + j, 1), :].astype(F32)
            gb_s[layer, 2 * i + j] = jnp.broadcast_to(row, (128, D)).T


def turn_weights(raw, turned):
    wo_r, wu_r, wd_r = raw
    wo_s, wu_s, wd_s = turned
    pieces = [lambda: wo_s.__setitem__(..., wo_r[...].T)]
    for c in range(0, F, D):
        pieces.append(lambda c=c: wu_s.__setitem__((pl.ds(c, D), slice(None)), wu_r[:, c:c + D].T * 0.5))
        pieces.append(lambda c=c: wd_s.__setitem__((slice(None), pl.ds(c, D)), wd_r[pl.ds(c, D), :].T))
    return pieces


def block_step(i, layer, xn, wqkv, turned, gb_s, x_s, a_s, qk_s, v_s, o_s, u_s, a2_s, xf_s, hf_s, mlp=True, att=True, extra=()):
    wo_s, wu_s, wd_s = turned
    extra = list(extra)
    cur = band(i, 1)
    nxt = 1 - cur
    zs, ss, es, os = {}, {}, {}, {}
    qc, qn = qk_s.at[cur], qk_s.at[nxt]
    an, a_out = a_s.at[nxt], a_s.at[cur]
    op, on = o_s.at[nxt], o_s.at[cur]

    def up(j):
        if not mlp: return
        zs[j] = [dot(wu_s[pl.ds(256 * j + 128 * t, 128), :], a2_s[...]) for t in range(2)]

    def act(j):
        if not mlp: return
        for t, z in enumerate(zs.pop(j)):
            u_s[pl.ds(256 * j + 128 * t, 128), :] = gelu_of_half(z)

    def lanes(h):
        return pl.ds(128 * (h // 3), 128)

    def S(h):
        if not att: return
        if layer == 0:
            ss[h] = dot(qc[pl.ds(D + h * DH, DH), :].T, qc[pl.ds(h * DH, DH), :])
        else:
            c, r = lanes(h), 128 * (h % 3)
            q0, q1 = qc[pl.ds(r, 64), c], qc[pl.ds(r + 64, 64), c]
            z = jnp.zeros_like(q0)
            q = jnp.concatenate([jnp.concatenate([q0, z], axis=1), jnp.concatenate([z, q1], axis=1)], axis=0)
            ss[h] = dot(qc[pl.ds(D + r, 128), c].T, q)

    def Pm(h):
        if not att: return
        s = ss.pop(h)
        e0, l0 = softmax_half(s[:, :128])
        e1, l1 = softmax_half(s[:, 128:])
        es[h] = (jnp.concatenate([e0, e1], axis=1), jnp.concatenate([l0, l1], axis=1))

    def PV(h):
        if not att: return
        if layer == 0:
            os[h] = dot(v_s[band(i, 3), pl.ds(h * DH, DH), :], es[h][0])
        else:
            os[h] = dot(v_s[band(i, 3), pl.ds(128 * (h % 3), 128), lanes(h)], es[h][0])

    def OS(h):
        if not att: return
        o, r = os.pop(h), 1.0 / es.pop(h)[1]
        if layer == 0:
            on[pl.ds(h * DH, DH), :] = (o * r).astype(BF)
        else:
            k, c = 128 * (h % 3), lanes(h)
            on[pl.ds(k, 64), c] = (o[:64, :128] * r[:, :128]).astype(BF)
            on[pl.ds(k + 64, 64), c] = (o[64:, 128:] * r[:, 128:]).astype(BF)

    def Q(c):
        if not att: return
        for t in range(2):
            r = dot(wqkv[pl.ds(c * D + 192 * t, 192), :], (an if c < 2 else a_out)[...]).astype(BF)
            if c < 2:
                qn[pl.ds(c * D + 192 * t, 192), :] = r
            else:
                v_s[band(i + 2, 3), pl.ds(192 * t, 192), :] = r

    def dn(k):
        if not mlp: return None
        return [dot(wd_s[pl.ds(192 * t, 192), 256 * k:256 * k + 256], u_s[pl.ds(256 * k, 256), :]) for t in range(2)]

    def fill(k=1):
        for _ in range(k):
            if extra: extra.pop(0)()

    def addl(*parts):
        if not mlp: return None
        return [functools.reduce(lambda a, b: a + b, z) for z in zip(*parts)]

    if mlp:
        pr = jnp.concatenate([dot(wo_s[pl.ds(192 * t, 192), :], op[...]) for t in range(2)], axis=0)
    S(0)
    Q(0)
    S(1); Pm(0)
    fill()
    if mlp: mean2 = ln2_p1(x_s.at[band(i + 3, 3)], pr, hf_s)
    Q(1)
    fill()
    if mlp: rstd2 = ln_p2(hf_s, mean2)
    PV(0)
    fill()
    if mlp: ln_p3(hf_s, mean2, rstd2, gb_s.at[layer, 1], gb_s.at[layer, 3], a2_s)
    up(0)
    Pm(1)
    S(2)
    up(1); act(0)
    OS(0); PV(1)
    fill()
    up(2); act(1)
    Pm(2); S(3); up(3)
    if att: mean1 = ln_p1(xn(), x_s.at[band(i + 2, 3)], xf_s)
    fill()
    PV(2); OS(1); act(2)
    if att: rstd1 = ln_p2(xf_s, mean1)
    Pm(3); S(4); up(4)
    fill()
    PV(3); OS(2); act(3)
    if att: ln_p3(xf_s, mean1, rstd1, gb_s.at[layer, 0], gb_s.at[layer, 2], a_out)
    Pm(4); S(5); up(5)
    PV(4); OS(3); act(4)
    fill()
    yd = addl(dn(0), dn(1))
    Pm(5)
    act(5)
    yd = addl(yd, dn(2), dn(3))
    PV(5); OS(4)
    fill(len(extra))
    yd = addl(yd, dn(4), dn(5))
    Q(2)
    OS(5)
    return (hf_s[...] + jnp.concatenate(yd, axis=0)).T.astype(BF) if mlp else None


def prologue(xns, wqkv, layer, gb_s, x_s, a_s, qk_s, v_s, xf_s):
    for t in range(2):
        mean = ln_p1(xns[t](), x_s.at[t], xf_s)
        ln_p3(xf_s, mean, ln_p2(xf_s, mean), gb_s.at[layer, 0], gb_s.at[layer, 2], a_s.at[t])
        for c in range(0 if t == 0 else 2 * D, 3 * D, 192):
            r = dot(wqkv[pl.ds(c, 192), :], a_s[t]).astype(BF)
            if c < 2 * D:
                qk_s[0, pl.ds(c, 192), :] = r
            else:
                v_s[t, pl.ds(c - 2 * D, 192), :] = r


NSLOT = 16
LAG = 8
STEPS = 32
EARLY = 48


def kernel(axis, n, x_ref, gain_ref, bias_ref, wqkv_ref, wout_ref, wup_ref, wdown_ref, z_ref, w_ref,
           wq_s, wo_r, wu_r, wd_r, wo_s, wu_s, wd_s, gb_s, x_s, a_s, qk_s, v_s, o_s, u_s, a2_s, xf_s, hf_s,
           xbuf, ybuf, zbuf, c_s, w_sem, x_sem, z_sem, local_sem, send_sem, late_sem, recv_sem):
    me = lax.axis_index(axis)
    peers = [lax.rem(me + k, n) for k in range(1, n)]
    barrier = pltpu.get_barrier_semaphore()
    for p in peers:
        pl.semaphore_signal(barrier, inc=1, device_id={axis: p}, device_id_type=MESH_ID)

    def x_copy(t):
        slot = band(t, 3)
        return pltpu.make_async_copy(x_ref.at[t], xbuf.at[slot], x_sem.at[slot])

    def w_copies(layer):
        pairs = ((wqkv_ref, wq_s), (wout_ref, wo_r), (wup_ref, wu_r), (wdown_ref, wd_r))
        return [pltpu.make_async_copy(h.at[layer], v.at[layer], w_sem.at[layer, j]) for j, (h, v) in enumerate(pairs)]

    first = w_copies(0)
    x_copy(0).start()
    first[0].start()
    for t in range(1, 4):
        x_copy(t).start()
    for c in first[1:] + w_copies(1):
        c.start()
    norm_rows(gain_ref, bias_ref, gb_s, 0)
    norm_rows(gain_ref, bias_ref, gb_s, 1)

    def turned(layer):
        return wo_s.at[layer], wu_s.at[layer], wd_s.at[layer]

    def raw(layer):
        return wo_r.at[layer], wu_r.at[layer], wd_r.at[layer]

    def step(i, layer, xn, **kw):
        return block_step(i, layer, xn, wq_s.at[layer], turned(layer), gb_s, x_s, a_s, qk_s, v_s, o_s, u_s, a2_s, xf_s, hf_s, **kw)

    part = T // n

    def patches(slot, p, start, size):
        return ybuf.at[slot, lax.shift_right_logical(p, 1), pl.ds(pl.multiple_of(part * band(p, 1) + start, 16), size)]

    def space_early(f, slot):
        out = [pltpu.make_async_copy(patches(slot, me, 0, part), z_ref.at[me * STEPS + f], local_sem.at[slot])]
        for k, p in enumerate(peers):
            out.append(pltpu.make_async_remote_copy(
                src_ref=patches(slot, p, 0, EARLY),
                dst_ref=z_ref.at[me * STEPS + f, pl.ds(0, EARLY)],
                send_sem=send_sem.at[slot, k], recv_sem=recv_sem.at[0, k], device_id={axis: p}, device_id_type=MESH_ID))
        return out

    def space_late(f, slot):
        return [pltpu.make_async_remote_copy(
            src_ref=patches(slot, p, EARLY, part - EARLY),
            dst_ref=z_ref.at[me * STEPS + f, pl.ds(EARLY, part - EARLY)],
            send_sem=late_sem.at[slot, k], recv_sem=recv_sem.at[1, k], device_id={axis: p}, device_id_type=MESH_ID)
            for k, p in enumerate(peers)]

    def sent(copies, local=True):
        if local:
            copies[0].wait()
            copies = copies[1:]
        for c in copies:
            c.wait_send()

    def slot_of(f):
        return band(f, NSLOT - 1)

    x_copy(0).wait()
    first[0].wait()
    x_copy(1).wait()
    prologue([lambda: xbuf[0].T, lambda: xbuf[1].T], wq_s.at[0], 0, gb_s, x_s, a_s, qk_s, v_s, xf_s)
    x_copy(2).wait()
    for c in first[1:]:
        c.wait()
    step(0, 0, lambda: xbuf[2].T, mlp=False, extra=turn_weights(raw(0), turned(0)))
    x_copy(4).start()
    pl.semaphore_wait(barrier, n - 1)

    def space_send(f):
        for c in space_early(f, slot_of(f)):
            c.start()

        @pl.when(f >= LAG)
        def _():
            for c in space_late(f - LAG, slot_of(f - LAG)):
                c.start()

    def space_step(i, _):
        f = i - 1

        @pl.when(i + 4 < STEPS)
        def _():
            x_copy(i + 4).start()

        @pl.when(i + 2 < STEPS)
        def _():
            x_copy(i + 2).wait()

        @pl.when(f >= NSLOT)
        def _():
            sent(space_early(f - NSLOT, slot_of(f)))
            sent(space_late(f - NSLOT, slot_of(f)), local=False)

        ybuf[slot_of(f)] = step(i, 0, lambda: xbuf[band(i + 2, 3)].T).reshape(2, 128, D)
        space_send(f)
        return 0

    lax.fori_loop(1, STEPS, space_step, 0)
    last = STEPS - 1
    sent(space_early(last - NSLOT, slot_of(last)))
    sent(space_late(last - NSLOT, slot_of(last)), local=False)
    ybuf[slot_of(last)] = step(STEPS, 0, None, att=False).reshape(2, 128, D)
    space_send(last)
    for f in range(STEPS - LAG, STEPS):
        for c in space_late(f, f % NSLOT):
            c.start()

    for c in w_copies(1):
        c.wait()
    for piece in turn_weights(raw(1), turned(1)):
        piece()
    for b in range(NSLOT):
        space_early(STEPS - NSLOT + b, b)[0].wait()
    for k in range(n - 1):
        got = z_ref.at[pl.ds(0, STEPS), pl.ds(0, EARLY)]
        pltpu.make_async_copy(got, got, recv_sem.at[0, k]).wait()

    def z_copy(c):
        slot = band(c, 1)
        return pltpu.make_async_copy(z_ref.at[:, pl.ds(pl.multiple_of(8 * c, 8), 8)], zbuf.at[slot], z_sem.at[slot])

    def convert(c, q):
        slot = band(c, 1)
        v = zbuf[slot, pl.ds(pl.multiple_of(32 * q, 32), 32)].astype(F32).reshape(256, D)
        for j in range(3):
            c_s[slot, j, pl.ds(pl.multiple_of(256 * q, 256), 256), :] = v[:, 128 * j:128 * j + 128]

    def tile(t):
        slot, pair = band((t // 4 if isinstance(t, int) else lax.shift_right_logical(t, 2)), 1), band(t, 3)
        return jnp.concatenate([
            jnp.concatenate([c_s[slot, j, pl.ds(2 * pair + b, 128, stride=8), :].astype(BF).T for b in range(2)], axis=1)
            for j in range(3)], axis=0)

    z_copy(0).start()
    z_copy(1).start()
    z_copy(0).wait()
    for q in range(4):
        convert(0, q)
    prologue([lambda: tile(0), lambda: tile(1)], wq_s.at[1], 1, gb_s, x_s, a_s, qk_s, v_s, xf_s)
    z_copy(1).wait()
    step(0, 1, lambda: tile(2), mlp=False, extra=[lambda q=q: convert(1, q) for q in range(3)])
    z_copy(2).start()

    rows = 128 // n

    def time_copies(f, slot):
        dst = w_ref.at[pl.ds(2 * (me * STEPS + f), 2)]
        out = [pltpu.make_async_copy(ybuf.at[slot, :, pl.ds(pl.multiple_of(rows * me, rows), rows)], dst, local_sem.at[slot])]
        for k, p in enumerate(peers):
            out.append(pltpu.make_async_remote_copy(
                src_ref=ybuf.at[slot, :, pl.ds(pl.multiple_of(rows * p, rows), rows)], dst_ref=dst,
                send_sem=send_sem.at[slot, k], recv_sem=recv_sem.at[2, k], device_id={axis: p}, device_id_type=MESH_ID))
        return out

    def reuse(f, slot):
        @pl.when(f < NSLOT)
        def _():
            sent(space_early(STEPS - NSLOT + f, slot)[1:], local=False)
            sent(space_late(STEPS - NSLOT + f, slot), local=False)

        @pl.when(f >= NSLOT)
        def _():
            sent(time_copies(f - NSLOT, slot))

    def time_step(i, _):
        f, t = i - 1, i + 2
        c = (t // 4 if isinstance(t, int) else lax.shift_right_logical(t, 2))

        @pl.when(jnp.logical_and(band(t, 3) == 0, c + 1 < 8))
        def _():
            z_copy(c + 1).wait()

            @pl.when(c + 2 == EARLY // 8)
            def _():
                for k in range(n - 1):
                    got = z_ref.at[pl.ds(0, STEPS), pl.ds(EARLY, part - EARLY)]
                    pltpu.make_async_copy(got, got, recv_sem.at[1, k]).wait()

            @pl.when(c + 2 < 8)
            def _():
                z_copy(c + 2).start()

        reuse(f, slot_of(f))
        convert(c + 1, band(t, 3))
        ybuf[slot_of(f)] = step(i, 1, lambda: tile(t)).reshape(2, 128, D)
        for cp in time_copies(f, slot_of(f)):
            cp.start()
        return 0

    lax.fori_loop(1, STEPS, time_step, 0)
    sent(time_copies(last - NSLOT, slot_of(last)))
    ybuf[slot_of(last)] = step(STEPS, 1, None, att=False).reshape(2, 128, D)
    for cp in time_copies(last, slot_of(last)):
        cp.start()
    for b in range(NSLOT):
        sent(time_copies(STEPS - NSLOT + b, b))
    for k in range(n - 1):
        got = w_ref.at[pl.ds(0, 2 * STEPS)]
        pltpu.make_async_copy(got, got, recv_sem.at[2, k]).wait()


def swap_kernel(w_ref, out_ref, perm_s):
    @pl.when(pl.program_id(0) == 0)
    def _():
        r, c = (lax.broadcasted_iota(jnp.int32, (T, T), d) for d in (0, 1))
        to = lax.shift_left(band(r, 15), 4) + lax.shift_right_logical(r, 4)
        perm_s[...] = jnp.where(to == c, 1.0, 0.0).astype(BF)

    for p in range(0, w_ref.shape[0], 16):
        for f in range(0, 32, 16):
            x = w_ref[pl.ds(p, 16), pl.ds(f, 16), :].reshape(T, D)
            out_ref[pl.ds(f, 16), pl.ds(p, 16), :] = dot(perm_s[...], x).astype(BF).reshape(16, 16, D)


def solution(mesh):
    axis = 'sp'
    n = mesh.shape[axis]
    act_spec = P('data', axis, None, None)
    hbm = pl.BlockSpec(memory_space=pl.ANY)
    vmem = pl.BlockSpec(memory_space=pltpu.VMEM)

    def local_run(latent, ln_gain, ln_bias, w_qkv, w_out, w_up, w_down):
        wqkv = jnp.transpose(w_qkv, (0, 2, 3, 4, 1)).reshape(2, 3 * D, D)
        _, w = pl.pallas_call(
            functools.partial(kernel, axis, n),
            out_shape=(jax.ShapeDtypeStruct((128, 64, D), BF), jax.ShapeDtypeStruct((256, 32, D), BF)),
            in_specs=[hbm, vmem, vmem, hbm, hbm, hbm, hbm],
            out_specs=(hbm, hbm),
            scratch_shapes=[
                pltpu.VMEM((2, 3 * D, D), BF), pltpu.VMEM((2, D, D), BF), pltpu.VMEM((2, D, F), BF), pltpu.VMEM((2, F, D), BF),
                pltpu.VMEM((2, D, D), BF), pltpu.VMEM((2, F, D), BF), pltpu.VMEM((2, D, F), BF),
                pltpu.VMEM((2, 4, D, 128), F32),
                pltpu.VMEM((4, D, T), BF), pltpu.VMEM((2, D, T), BF),
                pltpu.VMEM((2, 2 * D, T), BF), pltpu.VMEM((4, D, T), BF), pltpu.VMEM((2, D, T), BF), pltpu.VMEM((F, T), BF),
                pltpu.VMEM((D, T), BF),
                pltpu.VMEM((D, T), F32), pltpu.VMEM((D, T), F32),
                pltpu.VMEM((4, T, D), BF), pltpu.VMEM((NSLOT, 2, 128, D), BF),
                pltpu.VMEM((2, 128, 8, D), BF), pltpu.VMEM((2, 3, 1024, 128), F32),
                pltpu.SemaphoreType.DMA((2, 4)), pltpu.SemaphoreType.DMA((4,)), pltpu.SemaphoreType.DMA((2,)),
                pltpu.SemaphoreType.DMA((NSLOT,)), pltpu.SemaphoreType.DMA((NSLOT, n - 1)), pltpu.SemaphoreType.DMA((NSLOT, n - 1)),
                pltpu.SemaphoreType.DMA((3, n - 1)),
            ],
            compiler_params=pltpu.CompilerParams(
                vmem_limit_bytes=60 << 20, collective_id=0, has_side_effects=True),
            name='blocks',
        )(latent[0], ln_gain, ln_bias, wqkv, w_out.reshape(2, D, D), w_up, w_down)
        out = pl.pallas_call(
            swap_kernel,
            grid=(8,),
            out_shape=jax.ShapeDtypeStruct((32, 256, D), BF),
            in_specs=[pl.BlockSpec((32, 32, D), lambda i: (i, 0, 0))],
            out_specs=pl.BlockSpec((32, 32, D), lambda i: (0, i, 0)),
            scratch_shapes=[pltpu.VMEM((T, T), BF)],
            name='swap',
        )(w)
        return out[None]

    return jax.shard_map(local_run, mesh=mesh, in_specs=(act_spec, P(), P(), P(), P(), P(), P()), out_specs=act_spec, check_vma=False)
```

```python
import functools

import jax
import jax.numpy as jnp
from jax import lax
from jax.experimental import pallas as pl
from jax.experimental.pallas import tpu as pltpu
from jax.sharding import PartitionSpec as P

BF, F32 = jnp.bfloat16, jnp.float32
D, H, DH, F = 384, 6, 64, 1536
T = 256
EPS = 1e-6
C_EXP = 0.125 * 1.4426950408889634
G0, G1 = 0.7978845608028654, 0.044715
RB = 64
MESH_ID = pl.DeviceIdType.MESH


def band(a, b):
    return a & b if isinstance(a, int) else jnp.bitwise_and(a, b)


def dot(a, b):
    return jnp.dot(a, b, preferred_element_type=F32)


def psum(v):
    return jnp.sum(v.reshape(v.shape[0] // 8, 8, v.shape[1]), axis=0)


def dup(r):
    return jnp.concatenate([r, r], axis=1)


def full_mean(acc):
    return jnp.sum(acc, axis=0, keepdims=True) * (1.0 / D)


def gelu_of_half(z):
    return (z + z * jnp.tanh(z * (z * z * (8 * G0 * G1) + 2 * G0))).astype(BF)


def ln_p1(xn, x_ring, xf_s):
    x_ring[...] = xn
    acc = None
    for r in range(0, D, RB):
        f = xn[r:r + RB].astype(F32)
        xf_s[pl.ds(r, RB), :] = f
        t = psum(f)
        acc = t if acc is None else acc + t
    return full_mean(acc)


def ln2_p1(x_ring, pr, hf_s):
    acc = None
    for r in range(0, D, RB):
        f = (x_ring[pl.ds(r, RB), :].astype(F32) + pr[r:r + RB]).astype(BF).astype(F32)
        hf_s[pl.ds(r, RB), :] = f
        t = psum(f)
        acc = t if acc is None else acc + t
    return full_mean(acc)


def ln_p2(f_s, mean):
    acc = None
    for r in range(0, D, RB):
        c = f_s[pl.ds(r, RB), :] - mean
        t = psum(c * c)
        acc = t if acc is None else acc + t
    return lax.rsqrt(full_mean(acc) + EPS)


def ln_p3(f_s, mean, rstd, g_ref, b_ref, out):
    for r in range(0, D, RB):
        c = f_s[pl.ds(r, RB), :] - mean
        out[pl.ds(r, RB), :] = (c * rstd * dup(g_ref[pl.ds(r, RB), :]) + dup(b_ref[pl.ds(r, RB), :])).astype(BF)


def softmax_half(s):
    m = jnp.max(s, axis=0, keepdims=True)
    e = jnp.exp2((s - m) * C_EXP)
    return e.astype(BF), jnp.sum(e, axis=0, keepdims=True)


def norm_rows(gain_ref, bias_ref, gb_s, layer):
    for i, r in enumerate((gain_ref, bias_ref)):
        for j in range(2):
            row = r[pl.ds(2 * layer + j, 1), :].astype(F32)
            gb_s[layer, 2 * i + j] = jnp.broadcast_to(row, (128, D)).T


def turn_weights(raw, turned):
    wo_r, wu_r, wd_r = raw
    wo_s, wu_s, wd_s = turned
    pieces = [lambda: wo_s.__setitem__(..., wo_r[...].T)]
    for c in range(0, F, D):
        pieces.append(lambda c=c: wu_s.__setitem__((pl.ds(c, D), slice(None)), wu_r[:, c:c + D].T * 0.5))
        pieces.append(lambda c=c: wd_s.__setitem__((slice(None), pl.ds(c, D)), wd_r[pl.ds(c, D), :].T))
    return pieces


def block_step(i, layer, xn, wqkv, turned, gb_s, x_s, a_s, qk_s, v_s, o_s, u_s, a2_s, xf_s, hf_s, mlp=True, att=True, extra=()):
    wo_s, wu_s, wd_s = turned
    extra = list(extra)
    cur = band(i, 1)
    nxt = 1 - cur
    zs, ss, es, os = {}, {}, {}, {}
    qc, qn = qk_s.at[cur], qk_s.at[nxt]
    an, a_out = a_s.at[nxt], a_s.at[cur]
    op, on = o_s.at[nxt], o_s.at[cur]

    def up(j):
        if not mlp: return
        zs[j] = [dot(wu_s[pl.ds(256 * j + 128 * t, 128), :], a2_s[...]) for t in range(2)]

    def act(j):
        if not mlp: return
        for t, z in enumerate(zs.pop(j)):
            u_s[pl.ds(256 * j + 128 * t, 128), :] = gelu_of_half(z)

    def lanes(h):
        return pl.ds(128 * (h // 3), 128)

    def S(h):
        if not att: return
        if layer == 0:
            ss[h] = dot(qc[pl.ds(D + h * DH, DH), :].T, qc[pl.ds(h * DH, DH), :])
        else:
            c, r = lanes(h), 128 * (h % 3)
            q0, q1 = qc[pl.ds(r, 64), c], qc[pl.ds(r + 64, 64), c]
            z = jnp.zeros_like(q0)
            q = jnp.concatenate([jnp.concatenate([q0, z], axis=1), jnp.concatenate([z, q1], axis=1)], axis=0)
            ss[h] = dot(qc[pl.ds(D + r, 128), c].T, q)

    def Pm(h):
        if not att: return
        s = ss.pop(h)
        e0, l0 = softmax_half(s[:, :128])
        e1, l1 = softmax_half(s[:, 128:])
        es[h] = (jnp.concatenate([e0, e1], axis=1), jnp.concatenate([l0, l1], axis=1))

    def PV(h):
        if not att: return
        if layer == 0:
            os[h] = dot(v_s[band(i, 3), pl.ds(h * DH, DH), :], es[h][0])
        else:
            os[h] = dot(v_s[band(i, 3), pl.ds(128 * (h % 3), 128), lanes(h)], es[h][0])

    def OS(h):
        if not att: return
        o, r = os.pop(h), 1.0 / es.pop(h)[1]
        if layer == 0:
            on[pl.ds(h * DH, DH), :] = (o * r).astype(BF)
        else:
            k, c = 128 * (h % 3), lanes(h)
            on[pl.ds(k, 64), c] = (o[:64, :128] * r[:, :128]).astype(BF)
            on[pl.ds(k + 64, 64), c] = (o[64:, 128:] * r[:, 128:]).astype(BF)

    def Q(c):
        if not att: return
        for t in range(2):
            r = dot(wqkv[pl.ds(c * D + 192 * t, 192), :], (an if c < 2 else a_out)[...]).astype(BF)
            if c < 2:
                qn[pl.ds(c * D + 192 * t, 192), :] = r
            else:
                v_s[band(i + 2, 3), pl.ds(192 * t, 192), :] = r

    def dn(k):
        if not mlp: return None
        return [dot(wd_s[pl.ds(192 * t, 192), 256 * k:256 * k + 256], u_s[pl.ds(256 * k, 256), :]) for t in range(2)]

    def fill(k=1):
        for _ in range(k):
            if extra: extra.pop(0)()

    def addl(*parts):
        if not mlp: return None
        return [functools.reduce(lambda a, b: a + b, z) for z in zip(*parts)]

    if mlp:
        pr = jnp.concatenate([dot(wo_s[pl.ds(192 * t, 192), :], op[...]) for t in range(2)], axis=0)
    S(0)
    Q(0)
    S(1); Pm(0)
    fill()
    if mlp: mean2 = ln2_p1(x_s.at[band(i + 3, 3)], pr, hf_s)
    Q(1)
    fill()
    if mlp: rstd2 = ln_p2(hf_s, mean2)
    PV(0)
    fill()
    if mlp: ln_p3(hf_s, mean2, rstd2, gb_s.at[layer, 1], gb_s.at[layer, 3], a2_s)
    up(0)
    Pm(1)
    S(2)
    up(1); act(0)
    OS(0); PV(1)
    fill()
    up(2); act(1)
    Pm(2); S(3); up(3)
    if att: mean1 = ln_p1(xn(), x_s.at[band(i + 2, 3)], xf_s)
    fill()
    PV(2); OS(1); act(2)
    if att: rstd1 = ln_p2(xf_s, mean1)
    Pm(3); S(4); up(4)
    fill()
    PV(3); OS(2); act(3)
    if att: ln_p3(xf_s, mean1, rstd1, gb_s.at[layer, 0], gb_s.at[layer, 2], a_out)
    Pm(4); S(5); up(5)
    PV(4); OS(3); act(4)
    fill()
    yd = addl(dn(0), dn(1))
    Pm(5)
    act(5)
    yd = addl(yd, dn(2), dn(3))
    PV(5); OS(4)
    fill(len(extra))
    yd = addl(yd, dn(4), dn(5))
    Q(2)
    OS(5)
    return (hf_s[...] + jnp.concatenate(yd, axis=0)).T.astype(BF) if mlp else None


def prologue(xns, wqkv, layer, gb_s, x_s, a_s, qk_s, v_s, xf_s):
    for t in range(2):
        mean = ln_p1(xns[t](), x_s.at[t], xf_s)
        ln_p3(xf_s, mean, ln_p2(xf_s, mean), gb_s.at[layer, 0], gb_s.at[layer, 2], a_s.at[t])
        for c in range(0 if t == 0 else 2 * D, 3 * D, 192):
            r = dot(wqkv[pl.ds(c, 192), :], a_s[t]).astype(BF)
            if c < 2 * D:
                qk_s[0, pl.ds(c, 192), :] = r
            else:
                v_s[t, pl.ds(c - 2 * D, 192), :] = r


NSLOT = 16
STEPS = 32
EARLY = 6


def kernel(axis, n, x_ref, gain_ref, bias_ref, wqkv_ref, wout_ref, wup_ref, wdown_ref, w_ref,
           wq_s, wo_r, wu_r, wd_r, wo_s, wu_s, wd_s, gb_s, x_s, a_s, qk_s, v_s, o_s, u_s, a2_s, xf_s, hf_s,
           xbuf, ybuf, z_s, c_s, w_sem, x_sem, send_sem, late_sem, recv_sem):
    me = lax.axis_index(axis)
    peers = [lax.rem(me + k, n) for k in range(1, n)]
    barrier = pltpu.get_barrier_semaphore()
    for p in peers:
        pl.semaphore_signal(barrier, inc=1, device_id={axis: p}, device_id_type=MESH_ID)

    def x_copy(t):
        slot = band(t, 3)
        return pltpu.make_async_copy(x_ref.at[t], xbuf.at[slot], x_sem.at[slot])

    def w_copies(layer):
        pairs = ((wqkv_ref, wq_s), (wout_ref, wo_r), (wup_ref, wu_r), (wdown_ref, wd_r))
        return [pltpu.make_async_copy(h.at[layer], v.at[layer], w_sem.at[layer, j]) for j, (h, v) in enumerate(pairs)]

    first = w_copies(0)
    x_copy(0).start()
    first[0].start()
    for t in range(1, 4):
        x_copy(t).start()
    for c in first[1:] + w_copies(1):
        c.start()
    norm_rows(gain_ref, bias_ref, gb_s, 0)
    norm_rows(gain_ref, bias_ref, gb_s, 1)

    def turned(layer):
        return wo_s.at[layer], wu_s.at[layer], wd_s.at[layer]

    def raw(layer):
        return wo_r.at[layer], wu_r.at[layer], wd_r.at[layer]

    def step(i, layer, xn, **kw):
        return block_step(i, layer, xn, wq_s.at[layer], turned(layer), gb_s, x_s, a_s, qk_s, v_s, o_s, u_s, a2_s, xf_s, hf_s, **kw)

    def patches(slot, p, start, size):
        return ybuf.at[slot, lax.shift_right_logical(p, 1), pl.ds(8 * band(p, 1) + start, size)]

    def space_copies(f, start, size, send, part):
        return [pltpu.make_async_remote_copy(
            src_ref=patches(slot_of(f), p, start, size), dst_ref=z_s.at[me * STEPS + f, pl.ds(start, size)],
            send_sem=send.at[slot_of(f), k], recv_sem=recv_sem.at[part, k], device_id={axis: p}, device_id_type=MESH_ID)
            for k, p in enumerate(peers)]

    def space_early(f):
        return space_copies(f, 0, EARLY, send_sem, 0)

    def space_late(f):
        return space_copies(f, EARLY, 8 - EARLY, late_sem, 1)

    def sent(copies):
        for c in copies:
            c.wait_send()

    def slot_of(f):
        return band(f, NSLOT - 1)

    x_copy(0).wait()
    first[0].wait()
    x_copy(1).wait()
    prologue([lambda: xbuf[0].T, lambda: xbuf[1].T], wq_s.at[0], 0, gb_s, x_s, a_s, qk_s, v_s, xf_s)
    x_copy(2).wait()
    for c in first[1:]:
        c.wait()
    step(0, 0, lambda: xbuf[2].T, mlp=False, extra=turn_weights(raw(0), turned(0)))
    x_copy(4).start()
    pl.semaphore_wait(barrier, n - 1)

    def space_send(f):
        for c in space_early(f):
            c.start()
        z_s[me * STEPS + f] = patches(slot_of(f), me, 0, 8)[...]

    def space_step(i, _):
        f = i - 1

        @pl.when(i + 4 < STEPS)
        def _():
            x_copy(i + 4).start()

        @pl.when(i + 2 < STEPS)
        def _():
            x_copy(i + 2).wait()

        @pl.when(f >= NSLOT)
        def _():
            sent(space_early(f - NSLOT))
            sent(space_late(f - NSLOT))

        ybuf[slot_of(f)] = step(i, 0, lambda: xbuf[band(i + 2, 3)].T).reshape(2, 16, 8, D)
        space_send(f)

        @pl.when(lax.rem(f, 5) != 4)
        def _():
            for c in space_late(f - lax.div(f, 5)):
                c.start()
        return 0

    lax.fori_loop(1, STEPS, space_step, 0)
    last = STEPS - 1
    sent(space_early(last - NSLOT))
    sent(space_late(last - NSLOT))
    ybuf[slot_of(last)] = step(STEPS, 0, None, att=False).reshape(2, 16, 8, D)
    space_send(last)
    for f in range(last - last // 5, STEPS):
        for c in space_late(f):
            c.start()

    for c in w_copies(1):
        c.wait()
    for piece in turn_weights(raw(1), turned(1)):
        piece()
    for k in range(n - 1):
        got = z_s.at[pl.ds(0, STEPS), pl.ds(0, EARLY)]
        pltpu.make_async_copy(got, got, recv_sem.at[0, k]).wait()

    def convert(c, q):
        slot = band(c, 1)
        v = z_s[pl.ds(32 * q if isinstance(q, int) else pl.multiple_of(32 * q, 32), 32), c].astype(F32).reshape(256, D)
        for j in range(3):
            c_s[slot, j, pl.ds(256 * q if isinstance(q, int) else pl.multiple_of(256 * q, 256), 256), :] = v[:, 128 * j:128 * j + 128]

    def tile(t):
        slot, pair = band((t // 4 if isinstance(t, int) else lax.shift_right_logical(t, 2)), 1), band(t, 3)
        return jnp.concatenate([
            jnp.concatenate([c_s[slot, j, pl.ds(2 * pair + b, 128, stride=8), :].astype(BF).T for b in range(2)], axis=1)
            for j in range(3)], axis=0)

    for q in range(4):
        convert(0, q)
    prologue([lambda: tile(0), lambda: tile(1)], wq_s.at[1], 1, gb_s, x_s, a_s, qk_s, v_s, xf_s)
    step(0, 1, lambda: tile(2), mlp=False, extra=[lambda q=q: convert(1, q) for q in range(3)])

    def frames(slot, p):
        return ybuf.at[slot, :, pl.ds(4 * p, 4)]

    def time_copies(f):
        return [pltpu.make_async_remote_copy(
            src_ref=frames(slot_of(f), p), dst_ref=w_ref.at[pl.ds(2 * (me * STEPS + f), 2)],
            send_sem=send_sem.at[slot_of(f), k], recv_sem=recv_sem.at[2, k], device_id={axis: p}, device_id_type=MESH_ID)
            for k, p in enumerate(peers)]

    def time_send(f):
        for c in time_copies(f):
            c.start()
        w_ref[pl.ds(2 * (me * STEPS + f), 2)] = frames(slot_of(f), me)[...]

    def time_step(i, _):
        f, t = i - 1, i + 2

        @pl.when(t == 4 * (EARLY - 1))
        def _():
            for k in range(n - 1):
                got = z_s.at[pl.ds(0, STEPS), pl.ds(EARLY, 8 - EARLY)]
                pltpu.make_async_copy(got, got, recv_sem.at[1, k]).wait()

        @pl.when(f < NSLOT)
        def _():
            sent(space_early(STEPS - NSLOT + f))
            sent(space_late(STEPS - NSLOT + f))

        @pl.when(f >= NSLOT)
        def _():
            sent(time_copies(f - NSLOT))

        convert(jnp.minimum(lax.shift_right_logical(t, 2) + 1, 7), band(t, 3))
        ybuf[slot_of(f)] = step(i, 1, lambda: tile(t)).reshape(2, 16, 8, D)
        time_send(f)
        return 0

    lax.fori_loop(1, STEPS, time_step, 0)
    sent(time_copies(last - NSLOT))
    ybuf[slot_of(last)] = step(STEPS, 1, None, att=False).reshape(2, 16, 8, D)
    time_send(last)
    for f in range(STEPS - NSLOT, STEPS):
        sent(time_copies(f))
    for k in range(n - 1):
        got = w_ref.at[pl.ds(0, 2 * STEPS)]
        pltpu.make_async_copy(got, got, recv_sem.at[2, k]).wait()


def swap_kernel(w_ref, out_ref, out_s, sem):
    r, c = (lax.broadcasted_iota(jnp.int32, (T, T), d) for d in (0, 1))
    to = lax.shift_left(band(r, 15), 4) + lax.shift_right_logical(r, 4)
    perm = jnp.where(to == c, 1.0, 0.0).astype(BF)

    def copy(p):
        return pltpu.make_async_copy(out_s.at[p], out_ref.at[:, pl.ds(16 * p, 16)], sem.at[p])

    for p in range(16):
        for f in range(2):
            x = w_ref[pl.ds(16 * p, 16), pl.ds(2 * f, 2)].reshape(T, D)
            for h in range(2):
                out_s[p, pl.ds(16 * f + 8 * h, 8)] = dot(perm[128 * h:128 * h + 128], x).astype(BF).reshape(8, 16, D)
        copy(p).start()
    for p in range(16):
        copy(p).wait()


def solution(mesh):
    axis = 'sp'
    n = mesh.shape[axis]
    act_spec = P('data', axis, None, None)
    hbm = pl.BlockSpec(memory_space=pl.ANY)
    vmem = pl.BlockSpec(memory_space=pltpu.VMEM)

    def local_run(latent, ln_gain, ln_bias, w_qkv, w_out, w_up, w_down):
        wqkv = jnp.transpose(w_qkv, (0, 2, 3, 4, 1)).reshape(2, 3 * D, D)
        w = pl.pallas_call(
            functools.partial(kernel, axis, n),
            out_shape=pltpu.VMEM((256, 4, 8, D), BF),
            in_specs=[hbm, vmem, vmem, hbm, hbm, hbm, hbm],
            out_specs=vmem,
            scratch_shapes=[
                pltpu.VMEM((2, 3 * D, D), BF), pltpu.VMEM((2, D, D), BF), pltpu.VMEM((2, D, F), BF), pltpu.VMEM((2, F, D), BF),
                pltpu.VMEM((2, D, D), BF), pltpu.VMEM((2, F, D), BF), pltpu.VMEM((2, D, F), BF),
                pltpu.VMEM((2, 4, D, 128), F32),
                pltpu.VMEM((4, D, T), BF), pltpu.VMEM((2, D, T), BF),
                pltpu.VMEM((2, 2 * D, T), BF), pltpu.VMEM((4, D, T), BF), pltpu.VMEM((2, D, T), BF), pltpu.VMEM((F, T), BF),
                pltpu.VMEM((D, T), BF),
                pltpu.VMEM((D, T), F32), pltpu.VMEM((D, T), F32),
                pltpu.VMEM((4, T, D), BF), pltpu.VMEM((NSLOT, 2, 16, 8, D), BF),
                pltpu.VMEM((128, 8, 8, D), BF), pltpu.VMEM((2, 3, 1024, 128), F32),
                pltpu.SemaphoreType.DMA((2, 4)), pltpu.SemaphoreType.DMA((4,)),
                pltpu.SemaphoreType.DMA((NSLOT, n - 1)), pltpu.SemaphoreType.DMA((NSLOT, n - 1)),
                pltpu.SemaphoreType.DMA((3, n - 1)),
            ],
            compiler_params=pltpu.CompilerParams(
                vmem_limit_bytes=50 << 20, collective_id=0, has_side_effects=True),
            name='blocks',
        )(latent[0], ln_gain, ln_bias, wqkv, w_out.reshape(2, D, D), w_up, w_down)
        out = pl.pallas_call(
            swap_kernel,
            out_shape=jax.ShapeDtypeStruct((32, 256, D), BF),
            in_specs=[vmem],
            out_specs=hbm,
            scratch_shapes=[pltpu.VMEM((16, 32, 16, D), BF), pltpu.SemaphoreType.DMA((16,))],
            compiler_params=pltpu.CompilerParams(vmem_limit_bytes=40 << 20),
            name='swap',
        )(w)
        return out[None]

    return jax.shard_map(local_run, mesh=mesh, in_specs=(act_spec, P(), P(), P(), P(), P(), P()), out_specs=act_spec, check_vma=False)
```

```python
import functools

import jax
import jax.numpy as jnp
from jax import lax
from jax.experimental import pallas as pl
from jax.experimental.pallas import tpu as pltpu
from jax.sharding import PartitionSpec as P

BF, F32 = jnp.bfloat16, jnp.float32
D, H, DH, F = 384, 6, 64, 1536
T = 256
EPS = 1e-6
C_EXP = 0.125 * 1.4426950408889634
G0, G1 = 0.7978845608028654, 0.044715
RB = 64
MESH_ID = pl.DeviceIdType.MESH


def band(a, b):
    return a & b if isinstance(a, int) else jnp.bitwise_and(a, b)


def dot(a, b):
    return jnp.dot(a, b, preferred_element_type=F32)


def psum(v):
    return jnp.sum(v.reshape(v.shape[0] // 8, 8, v.shape[1]), axis=0)


def dup(r):
    return jnp.concatenate([r, r], axis=1)


def full_mean(acc):
    return jnp.sum(acc, axis=0, keepdims=True) * (1.0 / D)


def gelu_of_half(z):
    return (z + z * jnp.tanh(z * (z * z * (8 * G0 * G1) + 2 * G0))).astype(BF)


def ln_p1(xn, x_ring, xf_s):
    x_ring[...] = xn
    acc = None
    for r in range(0, D, RB):
        f = xn[r:r + RB].astype(F32)
        xf_s[pl.ds(r, RB), :] = f
        t = psum(f)
        acc = t if acc is None else acc + t
    return full_mean(acc)


def ln2_p1(x_ring, pr, hf_s):
    acc = None
    for r in range(0, D, RB):
        f = (x_ring[pl.ds(r, RB), :].astype(F32) + pr[r:r + RB]).astype(BF).astype(F32)
        hf_s[pl.ds(r, RB), :] = f
        t = psum(f)
        acc = t if acc is None else acc + t
    return full_mean(acc)


def ln_p2(f_s, mean):
    acc = None
    for r in range(0, D, RB):
        c = f_s[pl.ds(r, RB), :] - mean
        t = psum(c * c)
        acc = t if acc is None else acc + t
    return lax.rsqrt(full_mean(acc) + EPS)


def ln_p3(f_s, mean, rstd, g_ref, b_ref, out):
    for r in range(0, D, RB):
        c = f_s[pl.ds(r, RB), :] - mean
        out[pl.ds(r, RB), :] = (c * rstd * dup(g_ref[pl.ds(r, RB), :]) + dup(b_ref[pl.ds(r, RB), :])).astype(BF)


def softmax_half(s):
    m = jnp.max(s, axis=0, keepdims=True)
    e = jnp.exp2((s - m) * C_EXP)
    return e.astype(BF), jnp.sum(e, axis=0, keepdims=True)


def norm_rows(gain_ref, bias_ref, gb_s, layer):
    for i, r in enumerate((gain_ref, bias_ref)):
        for j in range(2):
            row = r[pl.ds(2 * layer + j, 1), :].astype(F32)
            gb_s[layer, 2 * i + j] = jnp.broadcast_to(row, (128, D)).T


def turn_weights(raw, turned):
    wo_r, wu_r, wd_r = raw
    wo_s, wu_s, wd_s = turned
    pieces = [lambda: wo_s.__setitem__(..., wo_r[...].T)]
    for c in range(0, F, D):
        pieces.append(lambda c=c: wu_s.__setitem__((pl.ds(c, D), slice(None)), wu_r[:, c:c + D].T * 0.5))
        pieces.append(lambda c=c: wd_s.__setitem__((slice(None), pl.ds(c, D)), wd_r[pl.ds(c, D), :].T))
    return pieces


def block_step(i, layer, xn, wqkv, turned, gb_s, x_s, a_s, qk_s, v_s, o_s, u_s, a2_s, xf_s, hf_s, cur, mlp=True, att=True, ahead=True, extra=()):
    wo_s, wu_s, wd_s = turned
    extra = list(extra)
    nxt = 1 - cur
    zs, ss, es, os = {}, {}, {}, {}
    qc, qn = qk_s.at[cur], qk_s.at[nxt]
    an, a_out = a_s.at[nxt], a_s.at[cur]
    op, on = o_s.at[nxt], o_s.at[cur]

    def up(j):
        if not mlp: return
        zs[j] = [dot(wu_s[pl.ds(256 * j + 128 * t, 128), :], a2_s[...]) for t in range(2)]

    def act(j):
        if not mlp: return
        for t, z in enumerate(zs.pop(j)):
            u_s[pl.ds(256 * j + 128 * t, 128), :] = gelu_of_half(z)

    def lanes(h):
        return pl.ds(128 * (h // 3), 128)

    def S(h):
        if not att: return
        if layer == 0:
            ss[h] = dot(qc[pl.ds(D + h * DH, DH), :].T, qc[pl.ds(h * DH, DH), :])
        else:
            c, r = lanes(h), 128 * (h % 3)
            q0, q1 = qc[pl.ds(r, 64), c], qc[pl.ds(r + 64, 64), c]
            z = jnp.zeros_like(q0)
            q = jnp.concatenate([jnp.concatenate([q0, z], axis=1), jnp.concatenate([z, q1], axis=1)], axis=0)
            ss[h] = dot(qc[pl.ds(D + r, 128), c].T, q)

    def Pm(h):
        if not att: return
        s = ss.pop(h)
        e0, l0 = softmax_half(s[:, :128])
        e1, l1 = softmax_half(s[:, 128:])
        es[h] = (jnp.concatenate([e0, e1], axis=1), jnp.concatenate([l0, l1], axis=1))

    def PV(h):
        if not att: return
        if layer == 0:
            os[h] = dot(v_s[band(i, 3), pl.ds(h * DH, DH), :], es[h][0])
        else:
            os[h] = dot(v_s[band(i, 3), pl.ds(128 * (h % 3), 128), lanes(h)], es[h][0])

    def OS(h):
        if not att: return
        o, r = os.pop(h), 1.0 / es.pop(h)[1]
        if layer == 0:
            on[pl.ds(h * DH, DH), :] = (o * r).astype(BF)
        else:
            k, c = 128 * (h % 3), lanes(h)
            on[pl.ds(k, 64), c] = (o[:64, :128] * r[:, :128]).astype(BF)
            on[pl.ds(k + 64, 64), c] = (o[64:, 128:] * r[:, 128:]).astype(BF)

    def Q(c):
        if not ahead: return
        for t in range(2):
            r = dot(wqkv[pl.ds(c * D + 192 * t, 192), :], (an if c < 2 else a_out)[...]).astype(BF)
            if c < 2:
                qn[pl.ds(c * D + 192 * t, 192), :] = r
            else:
                v_s[band(i + 2, 3), pl.ds(192 * t, 192), :] = r

    def dn(k):
        if not mlp: return None
        return [dot(wd_s[pl.ds(192 * t, 192), 256 * k:256 * k + 256], u_s[pl.ds(256 * k, 256), :]) for t in range(2)]

    def fill(k=1):
        for _ in range(k):
            if extra: extra.pop(0)()

    def addl(*parts):
        if not mlp: return None
        return [functools.reduce(lambda a, b: a + b, z) for z in zip(*parts)]

    if mlp:
        pr = jnp.concatenate([dot(wo_s[pl.ds(192 * t, 192), :], op[...]) for t in range(2)], axis=0)
    S(0)
    Q(0)
    S(1); Pm(0)
    fill()
    if mlp: mean2 = ln2_p1(x_s.at[band(i + 3, 3)], pr, hf_s)
    Q(1)
    fill()
    if mlp: rstd2 = ln_p2(hf_s, mean2)
    PV(0)
    fill()
    if mlp: ln_p3(hf_s, mean2, rstd2, gb_s.at[layer, 1], gb_s.at[layer, 3], a2_s)
    up(0)
    Pm(1)
    S(2)
    up(1); act(0)
    OS(0); PV(1)
    fill()
    up(2); act(1)
    Pm(2); S(3); up(3)
    if ahead: mean1 = ln_p1(xn(), x_s.at[band(i + 2, 3)], xf_s)
    fill()
    PV(2); OS(1); act(2)
    if ahead: rstd1 = ln_p2(xf_s, mean1)
    Pm(3); S(4); up(4)
    fill()
    PV(3); OS(2); act(3)
    if ahead: ln_p3(xf_s, mean1, rstd1, gb_s.at[layer, 0], gb_s.at[layer, 2], a_out)
    Pm(4); S(5); up(5)
    PV(4); OS(3); act(4)
    fill()
    yd = addl(dn(0), dn(1))
    Pm(5)
    act(5)
    yd = addl(yd, dn(2), dn(3))
    PV(5); OS(4)
    fill(len(extra))
    yd = addl(yd, dn(4), dn(5))
    Q(2)
    OS(5)
    return (hf_s[...] + jnp.concatenate(yd, axis=0)).T.astype(BF) if mlp else None


def prologue(xns, wqkv, layer, gb_s, x_s, a_s, qk_s, v_s, xf_s):
    for t in range(2):
        mean = ln_p1(xns[t](), x_s.at[t], xf_s)
        ln_p3(xf_s, mean, ln_p2(xf_s, mean), gb_s.at[layer, 0], gb_s.at[layer, 2], a_s.at[t])
        for c in range(0 if t == 0 else 2 * D, 3 * D, 192):
            r = dot(wqkv[pl.ds(c, 192), :], a_s[t]).astype(BF)
            if c < 2 * D:
                qk_s[0, pl.ds(c, 192), :] = r
            else:
                v_s[t, pl.ds(c - 2 * D, 192), :] = r


NSLOT = 16
STEPS = 32
STAGED = 4
EARLY = 6


def kernel(axis, n, x_ref, gain_ref, bias_ref, wqkv_ref, wout_ref, wup_ref, wdown_ref, w_ref,
           wq_s, wo_r, wu_r, wd_r, wo_s, wu_s, wd_s, gb_s, x_s, a_s, qk_s, v_s, o_s, u_s, a2_s, xf_s, hf_s,
           xbuf, ybuf, z_s, c_s, w_sem, x_sem, send_sem, late_sem, recv_sem):
    me = lax.axis_index(axis)
    peers = [lax.rem(me + k, n) for k in range(1, n)]
    barrier = pltpu.get_barrier_semaphore()
    for p in peers:
        pl.semaphore_signal(barrier, inc=1, device_id={axis: p}, device_id_type=MESH_ID)

    def x_copy(t):
        slot = band(t, 3)
        return pltpu.make_async_copy(x_ref.at[t], xbuf.at[slot], x_sem.at[slot])

    def w_copies(layer):
        pairs = ((wqkv_ref, wq_s), (wout_ref, wo_r), (wup_ref, wu_r), (wdown_ref, wd_r))
        return [pltpu.make_async_copy(h.at[layer], v.at[layer], w_sem.at[layer, j]) for j, (h, v) in enumerate(pairs)]

    first = w_copies(0)
    x_copy(0).start()
    first[0].start()
    for t in range(1, 4):
        x_copy(t).start()
    for c in first[1:] + w_copies(1):
        c.start()
    norm_rows(gain_ref, bias_ref, gb_s, 0)
    norm_rows(gain_ref, bias_ref, gb_s, 1)

    def turned(layer):
        return wo_s.at[layer], wu_s.at[layer], wd_s.at[layer]

    def raw(layer):
        return wo_r.at[layer], wu_r.at[layer], wd_r.at[layer]

    def slot_of(f):
        return band(f, NSLOT - 1)

    def step(i, layer, xn, cur, **kw):
        y = block_step(i, layer, xn, wq_s.at[layer], turned(layer), gb_s, x_s, a_s, qk_s, v_s, o_s, u_s, a2_s, xf_s, hf_s, cur, **kw)
        if y is not None:
            ybuf[slot_of(i - 1)] = y.reshape(2, 16, 8, D)

    def patches(slot, p, start, size):
        return ybuf.at[slot, lax.shift_right_logical(p, 1), pl.ds(8 * band(p, 1) + start, size)]

    def space_copies(f, start, size, send, part):
        return [pltpu.make_async_remote_copy(
            src_ref=patches(slot_of(f), p, start, size), dst_ref=z_s.at[me * STEPS + f, pl.ds(start, size)],
            send_sem=send.at[slot_of(f), k], recv_sem=recv_sem.at[part, k], device_id={axis: p}, device_id_type=MESH_ID)
            for k, p in enumerate(peers)]

    def space_early(f):
        return space_copies(f, 0, EARLY, send_sem, 0)

    def space_late(f):
        return space_copies(f, EARLY, 8 - EARLY, late_sem, 1)

    def sent(copies):
        for c in copies:
            c.wait_send()

    x_copy(0).wait()
    first[0].wait()
    x_copy(1).wait()
    prologue([lambda: xbuf[0].T, lambda: xbuf[1].T], wq_s.at[0], 0, gb_s, x_s, a_s, qk_s, v_s, xf_s)
    x_copy(2).wait()
    for c in first[1:]:
        c.wait()
    step(0, 0, lambda: xbuf[2].T, 0, mlp=False, extra=turn_weights(raw(0), turned(0)))
    x_copy(4).start()
    pl.semaphore_wait(barrier, n - 1)

    def space_send(f):
        for c in space_early(f):
            c.start()
        z_s[me * STEPS + f] = patches(slot_of(f), me, 0, 8)[...]

    def space_pair(j, _):
        i = 2 * j + 1
        f = i - 1

        @pl.when(i + 4 < STEPS)
        def _():
            x_copy(i + 4).start()

        @pl.when(i + 5 < STEPS)
        def _():
            x_copy(i + 5).start()

        @pl.when(i + 2 < STEPS)
        def _():
            x_copy(i + 2).wait()

        @pl.when(i + 3 < STEPS)
        def _():
            x_copy(i + 3).wait()

        @pl.when(f >= NSLOT)
        def _():
            for g in range(2):
                sent(space_early(f + g - NSLOT))
                sent(space_late(f + g - NSLOT))

        step(i, 0, lambda: xbuf[band(i + 2, 3)].T, 1)
        space_send(f)
        step(i + 1, 0, lambda: xbuf[band(i + 3, 3)].T, 0)
        space_send(f + 1)

        for g in range(2):
            @pl.when(lax.rem(f + g, 3) != 2)
            def _():
                for c in space_late(f + g - lax.div(f + g, 3)):
                    c.start()
        return 0

    lax.fori_loop(0, (STEPS - 1) // 2, space_pair, 0)
    last = STEPS - 1
    for f in (last - 1, last):
        sent(space_early(f - NSLOT))
        sent(space_late(f - NSLOT))
    step(last, 0, None, 1, ahead=False)
    space_send(last - 1)
    step(STEPS, 0, None, 0, att=False, ahead=False)
    space_send(last)
    left = list(range(last - 1 - (last - 1) // 3, STEPS))

    for c in w_copies(1):
        c.wait()
    for piece in turn_weights(raw(1), turned(1)):
        piece()
    for f in range(STEPS - STAGED, STEPS):
        sent(space_early(f))
        for g in left[:-(-len(left) // (STEPS - f))]:
            for c in space_late(g):
                c.start()
        left = left[-(-len(left) // (STEPS - f)):]
    for k in range(n - 1):
        got = z_s.at[pl.ds(0, STEPS), pl.ds(0, EARLY)]
        pltpu.make_async_copy(got, got, recv_sem.at[0, k]).wait()

    def convert(c, q):
        slot = band(c, 1)
        v = z_s[pl.ds(32 * q if isinstance(q, int) else pl.multiple_of(32 * q, 32), 32), c].astype(F32).reshape(256, D)
        for j in range(3):
            c_s[slot, j, pl.ds(256 * q if isinstance(q, int) else pl.multiple_of(256 * q, 256), 256), :] = v[:, 128 * j:128 * j + 128]

    def tile(t):
        slot, pair = band((t // 4 if isinstance(t, int) else lax.shift_right_logical(t, 2)), 1), band(t, 3)
        return jnp.concatenate([
            jnp.concatenate([c_s[slot, j, pl.ds(2 * pair + b, 128, stride=8), :].astype(BF).T for b in range(2)], axis=1)
            for j in range(3)], axis=0)

    for q in range(4):
        convert(0, q)
    prologue([lambda: tile(0), lambda: tile(1)], wq_s.at[1], 1, gb_s, x_s, a_s, qk_s, v_s, xf_s)
    step(0, 1, lambda: tile(2), 0, mlp=False, extra=[lambda q=q: convert(1, q) for q in range(3)])

    def frames(slot, p):
        return ybuf.at[slot, :, pl.ds(4 * p, 4)]

    def time_copies(f):
        return [pltpu.make_async_remote_copy(
            src_ref=frames(slot_of(f), p), dst_ref=w_ref.at[pl.ds(2 * (me * STEPS + f), 2)],
            send_sem=send_sem.at[slot_of(f), k], recv_sem=recv_sem.at[2, k], device_id={axis: p}, device_id_type=MESH_ID)
            for k, p in enumerate(peers)]

    def time_send(f):
        for c in time_copies(f):
            c.start()
        w_ref[pl.ds(2 * (me * STEPS + f), 2)] = frames(slot_of(f), me)[...]

    def time_pair(j, _):
        i = 2 * j + 1
        f, t = i - 1, i + 2

        @pl.when(t == 4 * (EARLY - 1) - 1)
        def _():
            for k in range(n - 1):
                got = z_s.at[pl.ds(0, STEPS), pl.ds(EARLY, 8 - EARLY)]
                pltpu.make_async_copy(got, got, recv_sem.at[1, k]).wait()

        @pl.when(f < NSLOT - STAGED)
        def _():
            for g in range(2):
                sent(space_early(STEPS - NSLOT + f + g))

        @pl.when(f < NSLOT)
        def _():
            for g in range(2):
                sent(space_late(STEPS - NSLOT + f + g))

        @pl.when(f >= NSLOT)
        def _():
            for g in range(2):
                sent(time_copies(f + g - NSLOT))

        for g in range(2):
            convert(jnp.minimum(lax.shift_right_logical(t + g, 2) + 1, 7), band(t + g, 3))
            step(i + g, 1, lambda: tile(t + g), 1 - g)
            time_send(f + g)
        return 0

    lax.fori_loop(0, (STEPS - 1) // 2, time_pair, 0)
    for f in (last - 1, last):
        sent(time_copies(f - NSLOT))
    step(last, 1, None, 1, ahead=False)
    time_send(last - 1)
    step(STEPS, 1, None, 0, att=False, ahead=False)
    time_send(last)
    for f in range(STEPS - NSLOT, STEPS):
        sent(time_copies(f))
    for k in range(n - 1):
        got = w_ref.at[pl.ds(0, 2 * STEPS)]
        pltpu.make_async_copy(got, got, recv_sem.at[2, k]).wait()


def swap_kernel(w_ref, out_ref, out_s, sem):
    r, c = (lax.broadcasted_iota(jnp.int32, (T, T), d) for d in (0, 1))
    to = lax.shift_left(band(r, 15), 4) + lax.shift_right_logical(r, 4)
    perm = jnp.where(to == c, 1.0, 0.0).astype(BF)

    def copy(p):
        return pltpu.make_async_copy(out_s.at[p], out_ref.at[:, pl.ds(16 * p, 16)], sem.at[p])

    for p in range(16):
        x = jnp.concatenate([w_ref[pl.ds(16 * p, 16), pl.ds(2 * f, 2)].reshape(T, D) for f in range(2)], axis=1)
        for h in range(2):
            y = dot(perm[128 * h:128 * h + 128], x).astype(BF)
            for f in range(2):
                out_s[p, pl.ds(16 * f + 8 * h, 8)] = y[:, D * f:D * f + D].reshape(8, 16, D)
        copy(p).start()
    for p in range(16):
        copy(p).wait()


def solution(mesh):
    axis = 'sp'
    n = mesh.shape[axis]
    act_spec = P('data', axis, None, None)
    hbm = pl.BlockSpec(memory_space=pl.ANY)
    vmem = pl.BlockSpec(memory_space=pltpu.VMEM)

    def local_run(latent, ln_gain, ln_bias, w_qkv, w_out, w_up, w_down):
        wqkv = jnp.transpose(w_qkv, (0, 2, 3, 4, 1)).reshape(2, 3 * D, D)
        w = pl.pallas_call(
            functools.partial(kernel, axis, n),
            out_shape=pltpu.VMEM((256, 4, 8, D), BF),
            in_specs=[hbm, vmem, vmem, hbm, hbm, hbm, hbm],
            out_specs=vmem,
            scratch_shapes=[
                pltpu.VMEM((2, 3 * D, D), BF), pltpu.VMEM((2, D, D), BF), pltpu.VMEM((2, D, F), BF), pltpu.VMEM((2, F, D), BF),
                pltpu.VMEM((2, D, D), BF), pltpu.VMEM((2, F, D), BF), pltpu.VMEM((2, D, F), BF),
                pltpu.VMEM((2, 4, D, 128), F32),
                pltpu.VMEM((4, D, T), BF), pltpu.VMEM((2, D, T), BF),
                pltpu.VMEM((2, 2 * D, T), BF), pltpu.VMEM((4, D, T), BF), pltpu.VMEM((2, D, T), BF), pltpu.VMEM((F, T), BF),
                pltpu.VMEM((D, T), BF),
                pltpu.VMEM((D, T), F32), pltpu.VMEM((D, T), F32),
                pltpu.VMEM((4, T, D), BF), pltpu.VMEM((NSLOT, 2, 16, 8, D), BF),
                pltpu.VMEM((128, 8, 8, D), BF), pltpu.VMEM((2, 3, 1024, 128), F32),
                pltpu.SemaphoreType.DMA((2, 4)), pltpu.SemaphoreType.DMA((4,)),
                pltpu.SemaphoreType.DMA((NSLOT, n - 1)), pltpu.SemaphoreType.DMA((NSLOT, n - 1)),
                pltpu.SemaphoreType.DMA((3, n - 1)),
            ],
            compiler_params=pltpu.CompilerParams(
                vmem_limit_bytes=50 << 20, collective_id=0, has_side_effects=True),
            name='blocks',
        )(latent[0], ln_gain, ln_bias, wqkv, w_out.reshape(2, D, D), w_up, w_down)
        out = pl.pallas_call(
            swap_kernel,
            out_shape=jax.ShapeDtypeStruct((32, 256, D), BF),
            in_specs=[vmem],
            out_specs=hbm,
            scratch_shapes=[pltpu.VMEM((16, 32, 16, D), BF), pltpu.SemaphoreType.DMA((16,))],
            compiler_params=pltpu.CompilerParams(vmem_limit_bytes=40 << 20),
            name='swap',
        )(w)
        return out[None]

    return jax.shard_map(local_run, mesh=mesh, in_specs=(act_spec, P(), P(), P(), P(), P(), P()), out_specs=act_spec, check_vma=False)
```

```python
import functools

import jax
import jax.numpy as jnp
from jax import lax
from jax.experimental import pallas as pl
from jax.experimental.pallas import tpu as pltpu
from jax.sharding import PartitionSpec as P

BF, F32 = jnp.bfloat16, jnp.float32
D, H, DH, F = 384, 6, 64, 1536
T = 256
EPS = 1e-6
C_EXP = 0.125 * 1.4426950408889634
G0, G1 = 0.7978845608028654, 0.044715
RB = 64
MESH_ID = pl.DeviceIdType.MESH


def band(a, b):
    return a & b if isinstance(a, int) else jnp.bitwise_and(a, b)


def dot(a, b):
    return jnp.dot(a, b, preferred_element_type=F32)


def psum(v):
    return jnp.sum(v.reshape(v.shape[0] // 8, 8, v.shape[1]), axis=0)


def dup(r):
    return jnp.concatenate([r, r], axis=1)


def full_mean(acc):
    return jnp.sum(acc, axis=0, keepdims=True) * (1.0 / D)


def gelu_of_half(z):
    return (z + z * jnp.tanh(z * (z * z * (8 * G0 * G1) + 2 * G0))).astype(BF)


def ln_p1(xn, x_ring, xf_s):
    x_ring[...] = xn
    acc = None
    for r in range(0, D, RB):
        f = xn[r:r + RB].astype(F32)
        xf_s[pl.ds(r, RB), :] = f
        t = psum(f)
        acc = t if acc is None else acc + t
    return full_mean(acc)


def ln2_p1(x_ring, pr, hf_s):
    acc = None
    for r in range(0, D, RB):
        f = (x_ring[pl.ds(r, RB), :].astype(F32) + pr[r:r + RB]).astype(BF).astype(F32)
        hf_s[pl.ds(r, RB), :] = f
        t = psum(f)
        acc = t if acc is None else acc + t
    return full_mean(acc)


def ln_p2(f_s, mean):
    acc = None
    for r in range(0, D, RB):
        c = f_s[pl.ds(r, RB), :] - mean
        t = psum(c * c)
        acc = t if acc is None else acc + t
    return lax.rsqrt(full_mean(acc) + EPS)


def ln_p3(f_s, mean, rstd, g_ref, b_ref, out):
    for r in range(0, D, RB):
        c = f_s[pl.ds(r, RB), :] - mean
        out[pl.ds(r, RB), :] = (c * rstd * dup(g_ref[pl.ds(r, RB), :]) + dup(b_ref[pl.ds(r, RB), :])).astype(BF)


def softmax_half(s):
    m = jnp.max(s, axis=0, keepdims=True)
    e = jnp.exp2((s - m) * C_EXP)
    return e.astype(BF), jnp.sum(e, axis=0, keepdims=True)


def norm_rows(gain_ref, bias_ref, gb_s, layer):
    for i, r in enumerate((gain_ref, bias_ref)):
        for j in range(2):
            row = r[pl.ds(2 * layer + j, 1), :].astype(F32)
            gb_s[layer, 2 * i + j] = jnp.broadcast_to(row, (128, D)).T


def turn_weights(raw, turned):
    wo_r, wu_r, wd_r = raw
    wo_s, wu_s, wd_s = turned
    pieces = [lambda: wo_s.__setitem__(..., wo_r[...].T)]
    for c in range(0, F, D):
        pieces.append(lambda c=c: wu_s.__setitem__((pl.ds(c, D), slice(None)), wu_r[:, c:c + D].T * 0.5))
        pieces.append(lambda c=c: wd_s.__setitem__((slice(None), pl.ds(c, D)), wd_r[pl.ds(c, D), :].T))
    return pieces


def block_step(i, layer, xn, wqkv, turned, gb_s, x_s, a_s, qk_s, v_s, o_s, u_s, a2_s, xf_s, hf_s, cur, mlp=True, att=True, ahead=True, extra=()):
    wo_s, wu_s, wd_s = turned
    extra = list(extra)
    nxt = 1 - cur
    zs, ss, es, os = {}, {}, {}, {}
    qc, qn = qk_s.at[cur], qk_s.at[nxt]
    an, a_out = a_s.at[nxt], a_s.at[cur]
    op, on = o_s.at[nxt], o_s.at[cur]

    def up(j):
        if not mlp: return
        zs[j] = [dot(wu_s[pl.ds(256 * j + 128 * t, 128), :], a2_s[...]) for t in range(2)]

    def act(j):
        if not mlp: return
        for t, z in enumerate(zs.pop(j)):
            u_s[pl.ds(256 * j + 128 * t, 128), :] = gelu_of_half(z)

    def lanes(h):
        return pl.ds(128 * (h // 3), 128)

    def S(h):
        if not att: return
        if layer == 0:
            ss[h] = dot(qc[pl.ds(D + h * DH, DH), :].T, qc[pl.ds(h * DH, DH), :])
        else:
            c, r = lanes(h), 128 * (h % 3)
            q0, q1 = qc[pl.ds(r, 64), c], qc[pl.ds(r + 64, 64), c]
            z = jnp.zeros_like(q0)
            q = jnp.concatenate([jnp.concatenate([q0, z], axis=1), jnp.concatenate([z, q1], axis=1)], axis=0)
            ss[h] = dot(qc[pl.ds(D + r, 128), c].T, q)

    def Pm(h):
        if not att: return
        s = ss.pop(h)
        e0, l0 = softmax_half(s[:, :128])
        e1, l1 = softmax_half(s[:, 128:])
        es[h] = (jnp.concatenate([e0, e1], axis=1), jnp.concatenate([l0, l1], axis=1))

    def PV(h):
        if not att: return
        if layer == 0:
            os[h] = dot(v_s[band(i, 3), pl.ds(h * DH, DH), :], es[h][0])
        else:
            os[h] = dot(v_s[band(i, 3), pl.ds(128 * (h % 3), 128), lanes(h)], es[h][0])

    def OS(h):
        if not att: return
        o, r = os.pop(h), 1.0 / es.pop(h)[1]
        if layer == 0:
            on[pl.ds(h * DH, DH), :] = (o * r).astype(BF)
        else:
            k, c = 128 * (h % 3), lanes(h)
            on[pl.ds(k, 64), c] = (o[:64, :128] * r[:, :128]).astype(BF)
            on[pl.ds(k + 64, 64), c] = (o[64:, 128:] * r[:, 128:]).astype(BF)

    def Q(c):
        if not ahead: return
        for t in range(2):
            r = dot(wqkv[pl.ds(c * D + 192 * t, 192), :], (an if c < 2 else a_out)[...]).astype(BF)
            if c < 2:
                qn[pl.ds(c * D + 192 * t, 192), :] = r
            else:
                v_s[band(i + 2, 3), pl.ds(192 * t, 192), :] = r

    def dn(k):
        if not mlp: return None
        return [dot(wd_s[pl.ds(192 * t, 192), 256 * k:256 * k + 256], u_s[pl.ds(256 * k, 256), :]) for t in range(2)]

    def fill(k=1):
        for _ in range(k):
            if extra: extra.pop(0)()

    def addl(*parts):
        if not mlp: return None
        return [functools.reduce(lambda a, b: a + b, z) for z in zip(*parts)]

    if mlp:
        pr = jnp.concatenate([dot(wo_s[pl.ds(192 * t, 192), :], op[...]) for t in range(2)], axis=0)
    S(0)
    Q(0)
    S(1); Pm(0)
    fill()
    if mlp: mean2 = ln2_p1(x_s.at[band(i + 3, 3)], pr, hf_s)
    Q(1)
    fill()
    if mlp: rstd2 = ln_p2(hf_s, mean2)
    PV(0)
    fill()
    if mlp: ln_p3(hf_s, mean2, rstd2, gb_s.at[layer, 1], gb_s.at[layer, 3], a2_s)
    up(0)
    Pm(1)
    S(2)
    up(1); act(0)
    OS(0); PV(1)
    fill()
    up(2); act(1)
    Pm(2); S(3); up(3)
    if ahead: mean1 = ln_p1(xn(), x_s.at[band(i + 2, 3)], xf_s)
    fill()
    PV(2); OS(1); act(2)
    if ahead: rstd1 = ln_p2(xf_s, mean1)
    Pm(3); S(4); up(4)
    fill()
    PV(3); OS(2); act(3)
    if ahead: ln_p3(xf_s, mean1, rstd1, gb_s.at[layer, 0], gb_s.at[layer, 2], a_out)
    Pm(4); S(5); up(5)
    PV(4); OS(3); act(4)
    fill()
    yd = addl(dn(0), dn(1))
    Pm(5)
    act(5)
    yd = addl(yd, dn(2), dn(3))
    PV(5); OS(4)
    fill(len(extra))
    yd = addl(yd, dn(4), dn(5))
    Q(2)
    OS(5)
    return (hf_s[...] + jnp.concatenate(yd, axis=0)).T.astype(BF) if mlp else None


def prologue(xns, wqkv, layer, gb_s, x_s, a_s, qk_s, v_s, xf_s):
    for t in range(2):
        mean = ln_p1(xns[t](), x_s.at[t], xf_s)
        ln_p3(xf_s, mean, ln_p2(xf_s, mean), gb_s.at[layer, 0], gb_s.at[layer, 2], a_s.at[t])
        for c in range(0 if t == 0 else 2 * D, 3 * D, 192):
            r = dot(wqkv[pl.ds(c, 192), :], a_s[t]).astype(BF)
            if c < 2 * D:
                qk_s[0, pl.ds(c, 192), :] = r
            else:
                v_s[t, pl.ds(c - 2 * D, 192), :] = r


NSLOT = 16
STEPS = 32
STAGED = 4
EARLY = 6


def kernel(axis, n, x_ref, gain_ref, bias_ref, wqkv_ref, wout_ref, wup_ref, wdown_ref, w_ref,
           wq_s, wo_r, wu_r, wd_r, wo_s, wu_s, wd_s, gb_s, x_s, a_s, qk_s, v_s, o_s, u_s, a2_s, xf_s, hf_s,
           xbuf, ybuf, z_s, c_s, w_sem, x_sem, send_sem, late_sem, recv_sem):
    me = lax.axis_index(axis)
    peers = [lax.rem(me + k, n) for k in range(1, n)]
    barrier = pltpu.get_barrier_semaphore()
    for p in peers:
        pl.semaphore_signal(barrier, inc=1, device_id={axis: p}, device_id_type=MESH_ID)

    def x_copy(t):
        slot = band(t, 3)
        return pltpu.make_async_copy(x_ref.at[t], xbuf.at[slot], x_sem.at[slot])

    def w_copies(layer):
        pairs = ((wqkv_ref, wq_s), (wout_ref, wo_r), (wup_ref, wu_r), (wdown_ref, wd_r))
        return [pltpu.make_async_copy(h.at[layer], v.at[layer], w_sem.at[layer, j]) for j, (h, v) in enumerate(pairs)]

    first, second = w_copies(0), w_copies(1)
    x_copy(0).start()
    first[0].start()
    x_copy(1).start()
    for c in first[1:]:
        c.start()
    for t in range(2, 4):
        x_copy(t).start()
    norm_rows(gain_ref, bias_ref, gb_s, 0)
    norm_rows(gain_ref, bias_ref, gb_s, 1)

    def turned(layer):
        return wo_s.at[layer], wu_s.at[layer], wd_s.at[layer]

    def raw(layer):
        return wo_r.at[layer], wu_r.at[layer], wd_r.at[layer]

    def slot_of(f):
        return band(f, NSLOT - 1)

    def step(i, layer, xn, cur, **kw):
        y = block_step(i, layer, xn, wq_s.at[layer], turned(layer), gb_s, x_s, a_s, qk_s, v_s, o_s, u_s, a2_s, xf_s, hf_s, cur, **kw)
        if y is not None:
            ybuf[slot_of(i - 1)] = y.reshape(2, 16, 8, D)

    def patches(slot, p, start, size):
        return ybuf.at[slot, lax.shift_right_logical(p, 1), pl.ds(8 * band(p, 1) + start, size)]

    def space_copies(f, start, size, send, part):
        return [pltpu.make_async_remote_copy(
            src_ref=patches(slot_of(f), p, start, size), dst_ref=z_s.at[me * STEPS + f, pl.ds(start, size)],
            send_sem=send.at[slot_of(f), k], recv_sem=recv_sem.at[part, k], device_id={axis: p}, device_id_type=MESH_ID)
            for k, p in enumerate(peers)]

    def space_early(f):
        return space_copies(f, 0, EARLY, send_sem, 0)

    def space_late(f):
        return space_copies(f, EARLY, 8 - EARLY, late_sem, 1)

    def sent(copies):
        for c in copies:
            c.wait_send()

    x_copy(0).wait()
    first[0].wait()
    x_copy(1).wait()
    prologue([lambda: xbuf[0].T, lambda: xbuf[1].T], wq_s.at[0], 0, gb_s, x_s, a_s, qk_s, v_s, xf_s)
    x_copy(2).wait()
    for c in first[1:]:
        c.wait()
    step(0, 0, lambda: xbuf[2].T, 0, mlp=False, extra=turn_weights(raw(0), turned(0)))
    x_copy(4).start()
    for c in second:
        c.start()
    pl.semaphore_wait(barrier, n - 1)

    def space_send(f):
        for c in space_early(f):
            c.start()
        z_s[me * STEPS + f] = patches(slot_of(f), me, 0, 8)[...]

    def space_pair(j, _):
        i = 2 * j + 1
        f = i - 1

        @pl.when(i + 4 < STEPS)
        def _():
            x_copy(i + 4).start()

        @pl.when(i + 5 < STEPS)
        def _():
            x_copy(i + 5).start()

        @pl.when(i + 2 < STEPS)
        def _():
            x_copy(i + 2).wait()

        @pl.when(i + 3 < STEPS)
        def _():
            x_copy(i + 3).wait()

        @pl.when(f >= NSLOT)
        def _():
            for g in range(2):
                sent(space_early(f + g - NSLOT))
                sent(space_late(f + g - NSLOT))

        step(i, 0, lambda: xbuf[band(i + 2, 3)].T, 1)
        space_send(f)
        step(i + 1, 0, lambda: xbuf[band(i + 3, 3)].T, 0)
        space_send(f + 1)

        for g in range(2):
            @pl.when(lax.rem(f + g, 3) != 2)
            def _():
                for c in space_late(f + g - lax.div(f + g, 3)):
                    c.start()
        return 0

    lax.fori_loop(0, (STEPS - 1) // 2, space_pair, 0)
    last = STEPS - 1
    for f in (last - 1, last):
        sent(space_early(f - NSLOT))
        sent(space_late(f - NSLOT))
    step(last, 0, None, 1, ahead=False)
    space_send(last - 1)
    step(STEPS, 0, None, 0, att=False, ahead=False)
    space_send(last)
    left = list(range(last - 1 - (last - 1) // 3, STEPS))

    for c in second:
        c.wait()
    for piece in turn_weights(raw(1), turned(1)):
        piece()
    for f in range(STEPS - STAGED, STEPS):
        sent(space_early(f))
        for g in left[:-(-len(left) // (STEPS - f))]:
            for c in space_late(g):
                c.start()
        left = left[-(-len(left) // (STEPS - f)):]
    for k in range(n - 1):
        got = z_s.at[pl.ds(0, STEPS), pl.ds(0, EARLY)]
        pltpu.make_async_copy(got, got, recv_sem.at[0, k]).wait()

    def convert(c, q):
        slot = band(c, 1)
        v = z_s[pl.ds(32 * q if isinstance(q, int) else pl.multiple_of(32 * q, 32), 32), c].astype(F32).reshape(256, D)
        for j in range(3):
            c_s[slot, j, pl.ds(256 * q if isinstance(q, int) else pl.multiple_of(256 * q, 256), 256), :] = v[:, 128 * j:128 * j + 128]

    def tile(t):
        slot, pair = band((t // 4 if isinstance(t, int) else lax.shift_right_logical(t, 2)), 1), band(t, 3)
        return jnp.concatenate([
            jnp.concatenate([c_s[slot, j, pl.ds(2 * pair + b, 128, stride=8), :].astype(BF).T for b in range(2)], axis=1)
            for j in range(3)], axis=0)

    for q in range(4):
        convert(0, q)
    prologue([lambda: tile(0), lambda: tile(1)], wq_s.at[1], 1, gb_s, x_s, a_s, qk_s, v_s, xf_s)
    step(0, 1, lambda: tile(2), 0, mlp=False, extra=[lambda q=q: convert(1, q) for q in range(3)])

    def frames(slot, p):
        return ybuf.at[slot, :, pl.ds(4 * p, 4)]

    def time_copies(f):
        return [pltpu.make_async_remote_copy(
            src_ref=frames(slot_of(f), p), dst_ref=w_ref.at[pl.ds(2 * (me * STEPS + f), 2)],
            send_sem=send_sem.at[slot_of(f), k], recv_sem=recv_sem.at[2, k], device_id={axis: p}, device_id_type=MESH_ID)
            for k, p in enumerate(peers)]

    def time_send(f):
        for c in time_copies(f):
            c.start()
        w_ref[pl.ds(2 * (me * STEPS + f), 2)] = frames(slot_of(f), me)[...]

    def time_pair(j, _):
        i = 2 * j + 1
        f, t = i - 1, i + 2

        @pl.when(t == 4 * (EARLY - 1) - 1)
        def _():
            for k in range(n - 1):
                got = z_s.at[pl.ds(0, STEPS), pl.ds(EARLY, 8 - EARLY)]
                pltpu.make_async_copy(got, got, recv_sem.at[1, k]).wait()

        @pl.when(f < NSLOT - STAGED)
        def _():
            for g in range(2):
                sent(space_early(STEPS - NSLOT + f + g))

        @pl.when(f < NSLOT)
        def _():
            for g in range(2):
                sent(space_late(STEPS - NSLOT + f + g))

        @pl.when(f >= NSLOT)
        def _():
            for g in range(2):
                sent(time_copies(f + g - NSLOT))

        for g in range(2):
            convert(jnp.minimum(lax.shift_right_logical(t + g, 2) + 1, 7), band(t + g, 3))
            step(i + g, 1, lambda: tile(t + g), 1 - g)
            time_send(f + g)
        return 0

    lax.fori_loop(0, (STEPS - 1) // 2, time_pair, 0)
    for f in (last - 1, last):
        sent(time_copies(f - NSLOT))
    step(last, 1, None, 1, ahead=False)
    time_send(last - 1)
    step(STEPS, 1, None, 0, att=False, ahead=False)
    time_send(last)
    for f in range(STEPS - NSLOT, STEPS):
        sent(time_copies(f))
    for k in range(n - 1):
        got = w_ref.at[pl.ds(0, 2 * STEPS)]
        pltpu.make_async_copy(got, got, recv_sem.at[2, k]).wait()


def swap_kernel(w_ref, out_ref, out_s, sem):
    r, c = (lax.broadcasted_iota(jnp.int32, (T, T), d) for d in (0, 1))
    to = lax.shift_left(band(r, 15), 4) + lax.shift_right_logical(r, 4)
    perm = jnp.where(to == c, 1.0, 0.0).astype(BF)

    def copy(p):
        return pltpu.make_async_copy(out_s.at[p], out_ref.at[:, pl.ds(16 * p, 16)], sem.at[p])

    for p in range(16):
        x = jnp.concatenate([w_ref[pl.ds(16 * p, 16), pl.ds(2 * f, 2)].reshape(T, D) for f in range(2)], axis=1)
        for h in range(2):
            y = dot(perm[128 * h:128 * h + 128], x).astype(BF)
            for f in range(2):
                out_s[p, pl.ds(16 * f + 8 * h, 8)] = y[:, D * f:D * f + D].reshape(8, 16, D)
        copy(p).start()
    for p in range(16):
        copy(p).wait()


def solution(mesh):
    axis = 'sp'
    n = mesh.shape[axis]
    act_spec = P('data', axis, None, None)
    hbm = pl.BlockSpec(memory_space=pl.ANY)
    vmem = pl.BlockSpec(memory_space=pltpu.VMEM)

    def local_run(latent, ln_gain, ln_bias, w_qkv, w_out, w_up, w_down):
        wqkv = jnp.transpose(w_qkv, (0, 2, 3, 4, 1)).reshape(2, 3 * D, D)
        w = pl.pallas_call(
            functools.partial(kernel, axis, n),
            out_shape=pltpu.VMEM((256, 4, 8, D), BF),
            in_specs=[hbm, vmem, vmem, hbm, hbm, hbm, hbm],
            out_specs=vmem,
            scratch_shapes=[
                pltpu.VMEM((2, 3 * D, D), BF), pltpu.VMEM((2, D, D), BF), pltpu.VMEM((2, D, F), BF), pltpu.VMEM((2, F, D), BF),
                pltpu.VMEM((2, D, D), BF), pltpu.VMEM((2, F, D), BF), pltpu.VMEM((2, D, F), BF),
                pltpu.VMEM((2, 4, D, 128), F32),
                pltpu.VMEM((4, D, T), BF), pltpu.VMEM((2, D, T), BF),
                pltpu.VMEM((2, 2 * D, T), BF), pltpu.VMEM((4, D, T), BF), pltpu.VMEM((2, D, T), BF), pltpu.VMEM((F, T), BF),
                pltpu.VMEM((D, T), BF),
                pltpu.VMEM((D, T), F32), pltpu.VMEM((D, T), F32),
                pltpu.VMEM((4, T, D), BF), pltpu.VMEM((NSLOT, 2, 16, 8, D), BF),
                pltpu.VMEM((128, 8, 8, D), BF), pltpu.VMEM((2, 3, 1024, 128), F32),
                pltpu.SemaphoreType.DMA((2, 4)), pltpu.SemaphoreType.DMA((4,)),
                pltpu.SemaphoreType.DMA((NSLOT, n - 1)), pltpu.SemaphoreType.DMA((NSLOT, n - 1)),
                pltpu.SemaphoreType.DMA((3, n - 1)),
            ],
            compiler_params=pltpu.CompilerParams(
                vmem_limit_bytes=50 << 20, collective_id=0, has_side_effects=True),
            name='blocks',
        )(latent[0], ln_gain, ln_bias, wqkv, w_out.reshape(2, D, D), w_up, w_down)
        out = pl.pallas_call(
            swap_kernel,
            out_shape=jax.ShapeDtypeStruct((32, 256, D), BF),
            in_specs=[vmem],
            out_specs=hbm,
            scratch_shapes=[pltpu.VMEM((16, 32, 16, D), BF), pltpu.SemaphoreType.DMA((16,))],
            compiler_params=pltpu.CompilerParams(vmem_limit_bytes=40 << 20),
            name='swap',
        )(w)
        return out[None]

    return jax.shard_map(local_run, mesh=mesh, in_specs=(act_spec, P(), P(), P(), P(), P(), P()), out_specs=act_spec, check_vma=False)
```
